32 devices in a mesh: pipe: 2 (over x), tensor: 4 (over y, core), seq: 4 (over z).
Axes of the slice: x: 2, y: 2, z: 4, core: 2. Of those that a mesh axis runs over, the one named last changes fastest.
Arguments:
- tokens: bfloat16 [2, 512, 2560], P(None, 'seq', 'tensor'), may hold values from -6 to 6
- prenorm_gain: float32 [2, 2560], P('pipe'), may hold values from 0.5 to 1.5
- gate_weight: bfloat16 [2, 2560, 5120], P('pipe', None, 'tensor'), may hold values from -0.125 to 0.125
- inner_weight: bfloat16 [2, 2560, 5120], P('pipe', None, 'tensor'), may hold values from -0.125 to 0.125
- state_weight: bfloat16 [2, 2560, 256], P('pipe'), may hold values from -0.125 to 0.125
- step_weight: bfloat16 [2, 2560, 80], P('pipe', None, 'tensor'), may hold values from -0.125 to 0.125
- inner_taps: float32 [2, 5, 5120], P('pipe', None, 'tensor'), may hold values from -3 to 3
- state_taps: float32 [2, 5, 256], P('pipe'), may hold values from -3 to 3
- step_bias: float32 [2, 80], P('pipe', 'tensor'), may hold values from -5 to -2
- decay_rate: float32 [2, 80], P('pipe', 'tensor'), may hold values from 0.001953125 to 1
- skip_scale: float32 [2, 80], P('pipe', 'tensor'), may hold values from 0.5 to 1.5
- inner_gain: float32 [2, 5120], P('pipe', 'tensor'), may hold values from 0.5 to 1.5
- out_weight: bfloat16 [2, 5120, 2560], P('pipe', 'tensor'), may hold values from -0.078125 to 0.078125
Outputs:
- layer_outputs: bfloat16 [2, 2, 512, 2560], P('pipe', None, 'seq', 'tensor')
The draws below stay inside these ranges and needn't reach their ends.
All inputs are finite; a program needn't handle non-finite values.
Results may differ from the reference program's by a relative error of at most 0.019.
Values may be sent and summed in bfloat16 or wider, within the bound.
A program may use at most 64 MiB of HBM per device.

```python
import math
import jax
import jax.numpy as jnp
from jax import lax

D = 2560
HEADS = 80
HEADDIM = 64
STATE = 128
KW = 4
BLOCK = 128
MICRO = 2
INNER = 5120
TOKENS = 512
LAYERS = 2


def block_levels(own_key, extent, cuts, least, top_value):
    level, own = 1.0, jax.random.fold_in(own_key, 6)
    for position, shards_of in cuts:
        steps = jnp.exp(jax.random.uniform(jax.random.fold_in(own, position), (shards_of,), jnp.float32, least / len(cuts), top_value / len(cuts)))
        level = level * jnp.repeat(steps, extent[position] // shards_of).reshape([-1 if axis == position else 1 for axis in range(len(extent))])
    return level


def gaussian(own_key, shape, scale, bound, shards=(), held_as=jnp.bfloat16):
    values = scale * jax.random.normal(own_key, shape, jnp.float32)
    if shards:
        values = values * block_levels(own_key, shape, shards, -0.22, 0.18)
    return jnp.clip(values, -bound, bound).astype(held_as)


def setup_inputs(seed: int = 0) -> dict:
    splits = jax.random.split(jax.random.key(seed), 14)
    return {
        "tokens": gaussian(splits[0], (MICRO, TOKENS, D), 1.0, 6.0, ((1, 4), (2, 4))),
        "prenorm_gain": jnp.clip(1.0 + 0.1 * jax.random.normal(splits[1], (LAYERS, D), jnp.float32), 0.5, 1.5),
        "gate_weight": gaussian(splits[2], (LAYERS, D, INNER), D ** -0.5, 0.125, ((0, 2), (2, 4))),
        "inner_weight": gaussian(splits[3], (LAYERS, D, INNER), D ** -0.5, 0.125, ((0, 2), (2, 4))),
        "state_weight": gaussian(splits[4], (LAYERS, D, 2 * STATE), D ** -0.5, 0.125, ((0, 2),)),
        "step_weight": gaussian(splits[5], (LAYERS, D, HEADS), D ** -0.5, 0.125, ((0, 2), (2, 4))),
        "inner_taps": gaussian(splits[6], (LAYERS, KW + 1, INNER), 0.5, 3.0, ((0, 2), (2, 4)), jnp.float32),
        "state_taps": gaussian(splits[7], (LAYERS, KW + 1, 2 * STATE), 0.5, 3.0, ((0, 2),), jnp.float32),
        "step_bias": jnp.clip(-5.0 + 3.0 * jax.random.uniform(splits[8], (LAYERS, HEADS), jnp.float32) ** block_levels(splits[8], (LAYERS, HEADS), ((0, 2), (1, 4)), -0.2, 0.2), -5.0, -2.0),
        "decay_rate": jnp.clip(jnp.exp(math.log(1.0) - 6.2383246 * jax.random.uniform(splits[9], (LAYERS, HEADS), jnp.float32) ** block_levels(splits[9], (LAYERS, HEADS), ((0, 2), (1, 4)), -0.2, 0.2)), 0.001953125, 1.0),
        "skip_scale": jnp.clip(0.5 + 1.0 * jax.random.uniform(splits[10], (LAYERS, HEADS), jnp.float32) ** block_levels(splits[10], (LAYERS, HEADS), ((0, 2), (1, 4)), -0.2, 0.2), 0.5, 1.5),
        "inner_gain": jnp.clip(1.0 + 0.1 * jax.random.normal(splits[11], (LAYERS, INNER), jnp.float32), 0.5, 1.5),
        "out_weight": gaussian(splits[12], (LAYERS, INNER, D), INNER ** -0.5, 0.078125, ((0, 2), (1, 4))),
    }


EPS = 1e-05

def causal_taps(values, taps):
    width = taps.shape[0] - 1
    length = values.shape[0]
    zeros = jnp.zeros((width - 1, values.shape[1]), values.dtype)
    padded = jnp.concatenate([zeros, values], axis=0).astype(jnp.float32)
    total = jnp.broadcast_to(taps[width][None, :], (length, values.shape[1]))
    for index in range(width):
        total = total + taps[index][None, :] * padded[index:index + length]
    return jax.nn.silu(total).astype(jnp.bfloat16)

def block_terms(inner_block, input_block, output_block, step_block, rate):
    size = step_block.shape[0]
    cumulative = jnp.cumsum(-step_block * rate[None, :], axis=0)
    by_head = cumulative.T
    later = jnp.arange(size)[:, None] >= jnp.arange(size)[None, :]
    decay = jnp.exp(jnp.where(later[None], by_head[:, :, None] - by_head[:, None, :], -jnp.inf))
    scores = jnp.dot(output_block, input_block.T, preferred_element_type=jnp.float32)
    mixing = (scores[None] * decay * step_block.T[:, None, :]).astype(jnp.bfloat16)
    inside = jnp.einsum('hqs,shp->qhp', mixing.astype(jnp.float32), inner_block.astype(jnp.float32))
    weighting = jnp.exp(cumulative[-1:] - cumulative) * step_block
    weighted = (inner_block.astype(jnp.float32) * weighting[:, :, None]).astype(jnp.bfloat16)
    state = jnp.einsum('shp,sn->hpn', weighted.astype(jnp.float32), input_block.astype(jnp.float32))
    return (cumulative, inside, state, jnp.exp(cumulative[-1]))

def state_space(inner_conv, state_conv, step_size, rate, skip):
    length = inner_conv.shape[0]
    count = length // BLOCK
    inner_blocks = inner_conv.reshape(count, BLOCK, HEADS, HEADDIM)
    input_blocks = state_conv[:, :STATE].reshape(count, BLOCK, STATE)
    output_blocks = state_conv[:, STATE:].reshape(count, BLOCK, STATE)
    step_blocks = step_size.reshape(count, BLOCK, HEADS)

    def advance(carried, items):
        inner_block, input_block, output_block, step_block = items
        cumulative, inside, state, decay = block_terms(inner_block, input_block, output_block, step_block, rate)
        across = jnp.exp(cumulative)[:, :, None] * jnp.einsum('qn,hpn->qhp', output_block.astype(jnp.float32), carried, precision=lax.Precision.HIGHEST)
        return (carried * decay[:, None, None] + state, inside + across)
    initial = jnp.zeros((HEADS, HEADDIM, STATE), jnp.float32)
    _, pieces = lax.scan(advance, initial, (inner_blocks, input_blocks, output_blocks, step_blocks))
    mixed = pieces + skip[None, None, :, None] * inner_blocks.astype(jnp.float32)
    return mixed.reshape(length, HEADS * HEADDIM)

def layer(current, prenorm, gate_weight, inner_weight, state_weight, step_weight, inner_taps, state_taps, step_bias, decay_rate, skip_scale, inner_gain, out_weight):
    widened = current.astype(jnp.float32)
    normed_in = (widened * lax.rsqrt(lax.optimization_barrier(jnp.mean(widened * widened, axis=1, keepdims=True)) + EPS) * prenorm).astype(jnp.bfloat16)
    gate_raw = jnp.dot(normed_in, gate_weight, preferred_element_type=jnp.float32).astype(jnp.bfloat16)
    inner_raw = jnp.dot(normed_in, inner_weight, preferred_element_type=jnp.float32).astype(jnp.bfloat16)
    state_raw = jnp.dot(normed_in, state_weight, preferred_element_type=jnp.float32).astype(jnp.bfloat16)
    step_raw = jnp.dot(normed_in, step_weight, preferred_element_type=jnp.float32)
    inner_conv = causal_taps(inner_raw, inner_taps)
    state_conv = causal_taps(state_raw, state_taps)
    step_size = jax.nn.softplus(step_raw + step_bias)
    mixed = state_space(inner_conv, state_conv, step_size, decay_rate, skip_scale)
    gated = mixed * jax.nn.silu(gate_raw.astype(jnp.float32))
    normed = (gated * lax.rsqrt(lax.optimization_barrier(jnp.mean(gated * gated, axis=1, keepdims=True)) + EPS) * inner_gain).astype(jnp.bfloat16)
    summed = jnp.dot(normed, out_weight, preferred_element_type=jnp.float32)
    return (widened + summed).astype(jnp.bfloat16)

def reference(tokens, prenorm_gain, gate_weight, inner_weight, state_weight, step_weight, inner_taps, state_taps, step_bias, decay_rate, skip_scale, inner_gain, out_weight):
    results = []
    for micro in range(MICRO):
        current = tokens[micro]
        per_layer = []
        for depth in range(LAYERS):
            current = layer(current, prenorm_gain[depth], gate_weight[depth], inner_weight[depth], state_weight[depth], step_weight[depth], inner_taps[depth], state_taps[depth], step_bias[depth], decay_rate[depth], skip_scale[depth], inner_gain[depth], out_weight[depth])
            per_layer.append(current)
        results.append(jnp.stack(per_layer))
    return jnp.stack(results, axis=1)
```

```python
import functools

import jax
import jax.numpy as jnp
from jax import lax
from jax.experimental import pallas as pl
from jax.experimental.pallas import tpu as pltpu
from jax.sharding import PartitionSpec as P

EPS = 1e-05
LANES = 128
MESH = pl.DeviceIdType.MESH
F32 = jnp.float32
BF16 = jnp.bfloat16


LOG2E = 1.4426950408889634
CAP = 126.0


def half_silu(h):
    return h + h * jnp.tanh(h)


def split(v, parts):
    pieces = []
    for _ in range(parts - 1):
        piece = v.astype(BF16)
        pieces.append(piece)
        v = v - piece.astype(F32)
    return pieces + [v.astype(BF16)]


def remote(src, dst, send, recv, where):
    return pltpu.make_async_remote_copy(
        src_ref=src, dst_ref=dst, send_sem=send, recv_sem=recv, device_id=where, device_id_type=MESH
    )


def kernel(
    sizes,
    tokens,
    prenorm_hbm,
    gate_hbm,
    inner_hbm,
    state_hbm,
    step_hbm,
    inner_taps_hbm,
    state_taps_hbm,
    step_bias_hbm,
    decay_rate_hbm,
    skip_scale_hbm,
    inner_gain_hbm,
    out_hbm,
    out,
    prenorm,
    inner_taps,
    state_taps,
    step_bias,
    decay_rate,
    skip_scale,
    inner_gain,
    w_gate,
    w_inner,
    w_state,
    w_step,
    w_out,
    u,
    ni,
    raw,
    conv,
    gate,
    rates,
    w_step_t,
    later3,
    spread_w,
    spread_c,
    skips,
    lhs_c,
    fall_t,
    weight_x,
    decay_x,
    scores,
    states,
    ent,
    snd,
    base,
    g,
    sq_acc,
    sq_own,
    sq_all,
    term,
    parts,
    own,
    w_sem,
    v_sem,
    t_sem,
    ag_send,
    ag_recv,
    rim_send,
    rim_recv,
    ch_send,
    ch_recv,
    rs_send,
    rs_recv,
    sq_send,
    sq_recv,
    pipe_send,
    pipe_recv,
):
    n_pipe, n_tensor, n_seq = sizes
    micros, rows, narrow = own.shape
    width = prenorm.shape[1]
    inner = w_inner.shape[1]
    heads = step_bias.shape[1]
    head_size = inner // heads
    pack = LANES // head_size
    pairs = inner // LANES
    tiles = raw.shape[1]
    reach = inner_taps.shape[0] - 2
    edge = raw.shape[2] - rows
    section = lax.axis_index("pipe")
    me = lax.axis_index("tensor")
    place = lax.axis_index("seq")
    half = LANES // 2
    wide = 2 * LANES

    loads = [
        pltpu.make_async_copy(src.at[0], dst, w_sem.at[k])
        for k, (src, dst) in enumerate(
            (
                (inner_hbm, w_inner),
                (state_hbm, w_state),
                (step_hbm, w_step),
                (gate_hbm, w_gate),
                (out_hbm, w_out),
            )
        )
    ]
    vectors = [
        pltpu.make_async_copy(src, dst, v_sem.at[k])
        for k, (src, dst) in enumerate(
            (
                (prenorm_hbm, prenorm),
                (inner_taps_hbm, inner_taps),
                (state_taps_hbm, state_taps),
                (step_bias_hbm, step_bias),
                (decay_rate_hbm, decay_rate),
                (skip_scale_hbm, skip_scale),
                (inner_gain_hbm, inner_gain),
            )
        )
    ]

    def stage(m):
        return pltpu.make_async_copy(tokens.at[m], u.at[m, me], t_sem.at[m])

    core = lax.rem(me, 2)
    partner = me + 1 - 2 * core
    chips = n_tensor // 2
    pieces = ag_send.shape[2]
    some = rows // pieces

    def at_chip(d):
        return 2 * lax.rem(me // 2 + d, chips) + core

    def gather(m, q, src, key, where):
        block = u.at[m, src, pl.ds(q * some, some)]
        return remote(
            block, block, ag_send.at[m, key, q], ag_recv.at[m, src, q], {"tensor": where}
        )

    def near(m, q):
        return gather(m, q, me, partner, partner)

    def cross(m, d, q):
        return gather(m, q, me, at_chip(d), at_chip(d))

    def hand(m, d, q):
        return gather(m, q, at_chip(d), at_chip(d) + 1 - 2 * core, partner)

    def gathered(m, q, src):
        return gather(m, q, src, src, partner)

    def send_own(m, q):
        for d in range(1, chips):
            cross(m, d, q).start()
        near(m, q).start()

    def rim_copy(m):
        return remote(
            raw.at[m, :, pl.ds(rows, edge)],
            raw.at[m, :, pl.ds(0, edge)],
            rim_send.at[m],
            rim_recv.at[m],
            {"seq": lax.rem(place + 1, n_seq)},
        )

    def chain(m, i):
        return remote(
            snd.at[m, i],
            ent.at[m, i],
            ch_send.at[m, i],
            ch_recv.at[m, i],
            {"seq": lax.rem(place + 1, n_seq)},
        )

    def part(m, j):
        return remote(
            term.at[m, j], parts.at[m, me], rs_send.at[m, j], rs_recv.at[m, me], {"tensor": j}
        )

    def parted(m, j):
        return remote(
            parts.at[m, j], parts.at[m, j], rs_send.at[m, j], rs_recv.at[m, j], {"tensor": j}
        )

    def squares(m, j):
        return remote(
            sq_own.at[m], sq_all.at[m, me], sq_send.at[m, j], sq_recv.at[m, me], {"tensor": j}
        )

    def squared(m, j):
        return remote(
            sq_all.at[m, j], sq_all.at[m, j], sq_send.at[m, j], sq_recv.at[m, j], {"tensor": j}
        )

    def relay(m, q):
        return remote(
            own.at[m, pl.ds(q * some, some)],
            u.at[m, me, pl.ds(q * some, some)],
            pipe_send.at[m, q],
            pipe_recv.at[m, q],
            {"pipe": lax.rem(section + 1, n_pipe)},
        )

    def others(action):
        for j in range(n_tensor):
            pl.when(me != j)(functools.partial(action, j))

    @pl.when(section == 0)
    def _():
        for m in range(micros):
            stage(m).start()

    for load in vectors + loads:
        load.start()

    barrier = pltpu.get_barrier_semaphore()

    def greet(where):
        pl.semaphore_signal(barrier, inc=1, device_id=where, device_id_type=MESH)

    others(lambda j: greet({"tensor": j}))
    partners = n_tensor - 1
    for axis, index, count in (("seq", place, n_seq), ("pipe", section, n_pipe)):
        pl.when(index > 0)(functools.partial(greet, {axis: index - 1}))
        pl.when(index < count - 1)(functools.partial(greet, {axis: index + 1}))
        partners = partners + jnp.where(index > 0, 1, 0) + jnp.where(index < count - 1, 1, 0)
    pl.semaphore_wait(barrier, partners)

    @pl.when(section == 0)
    def _():
        for m in range(micros):
            stage(m).wait()
        for q in range(pieces):
            send_own(0, q)

    for load in vectors:
        load.wait()
    inner_taps[...] = inner_taps[...] * 0.5
    state_taps[...] = state_taps[...] * 0.5
    rates[...] = jnp.zeros_like(rates)
    rates[0:1, :heads] = decay_rate[...] * (-LOG2E)
    rates[1:2, :heads] = step_bias[...]
    rates[2:3, :heads] = skip_scale[...]
    sq_acc[...] = jnp.zeros_like(sq_acc)

    @pl.when(place == 0)
    def _():
        for m in range(micros):
            raw[m, :, 0:edge, :] = jnp.zeros((tiles, edge, LANES), F32)
        ent[...] = jnp.zeros_like(ent)

    low = lax.broadcasted_iota(jnp.int32, (rows, LANES), 0)
    lane = lax.broadcasted_iota(jnp.int32, (rows, LANES), 1)
    later = low >= lane
    for k in range(3):
        later3[:, k * rows : (k + 1) * rows] = later.astype(F32).astype(BF16)

    def spreading(columns, size, first):
        k = lax.broadcasted_iota(jnp.int32, (wide, columns), 0)
        at = lax.broadcasted_iota(jnp.int32, (wide, columns), 1) + first
        row = k
        for start in (half, LANES, LANES + half):
            if size == head_size and start != LANES:
                continue
            row = jnp.where(k >= start, k - start, row)
        if size != head_size:
            row = jnp.where(jnp.logical_and(k >= half, k < LANES), LANES, row)
        inside = jnp.logical_and(at >= row * size, at < (row + 1) * size)
        return jnp.where(inside, 1.0, 0.0).astype(BF16)

    def fill_w(t, _):
        at = pl.multiple_of(t * LANES, LANES)
        spread_w[:, pl.ds(at, LANES)] = spreading(LANES, head_size, at)
        return 0

    def fill_c(t, _):
        at = pl.multiple_of(t * LANES, LANES)
        spread_c[:, pl.ds(at, LANES)] = spreading(LANES, rows, at)
        return 0

    lax.fori_loop(0, pairs, fill_w, 0)
    lax.fori_loop(0, heads, fill_c, 0)
    for t in range(pairs):
        cols = slice(t * LANES, (t + 1) * LANES)
        r = lax.broadcasted_iota(jnp.int32, (8, LANES), 0)
        whole = jnp.broadcast_to(rates[2:3], (8, LANES))
        h0 = lax.broadcasted_iota(jnp.int32, (8, LANES), 1)
        row = jnp.zeros((8, LANES), F32)
        for k in range(pack):
            one = jnp.sum(jnp.where(h0 == t * pack + k, whole, 0.0), axis=1, keepdims=True)
            row = jnp.where(h0 >= k * head_size, one, row)
        skips[:, cols] = row[0:1]

    def forward(m):
        for q in range(pieces):
            relay(m, q).wait_recv()
            send_own(m, q)

    def hand_over(m):
        for q in range(pieces):
            for d in range(1, chips):
                gathered(m, q, at_chip(d)).wait_recv()
                hand(m, d, q).start()

    def take_input(m):
        for q in range(pieces):
            gathered(m, q, partner).wait_recv()
            for d in range(1, chips):
                gathered(m, q, at_chip(d) + 1 - 2 * core).wait_recv()

        def norm(r, _):
            at = pl.ds(pl.multiple_of(r * 32, 32), 32)
            total = jnp.zeros((32, 1), F32)
            for j in range(n_tensor):
                v = u[m, j, at, :].astype(F32)
                total = total + jnp.sum(v * v, axis=1, keepdims=True)
            scale = lax.rsqrt(total / width + EPS)
            for j in range(n_tensor):
                cols = slice(j * narrow, (j + 1) * narrow)
                v = u[m, j, at, :].astype(F32)
                ni[m, at, cols] = (v * scale * prenorm[:, cols]).astype(BF16)
            return 0

        lax.fori_loop(0, rows // 32, norm, 0)

    def project(m):
        if m == 0:
            loads[0].wait()
            loads[1].wait()
            loads[2].wait()
            w_step_t[...] = jnp.zeros_like(w_step_t)
            padded = jnp.concatenate(
                [w_step[...].astype(F32), jnp.zeros((LANES - heads, width), F32)], axis=0
            )
            w_step_t[...] = padded.T.astype(BF16)

        def into(first, count, weights):
            for t in range(0, count, 2):
                end = min(t + 2, count)
                r = jnp.dot(
                    ni[m], weights[:, t * LANES : end * LANES], preferred_element_type=F32
                )
                for k in range(t, end):
                    raw[m, first + k, edge:, :] = r[:, (k - t) * LANES : (k - t + 1) * LANES]

        into(pairs, tiles - pairs, w_state)
        into(0, pairs, w_inner)
        v = jnp.dot(ni[m], w_step_t[...], preferred_element_type=F32) + rates[1:2]

        @pl.when(place < n_seq - 1)
        def _():
            rim_copy(m).start()

        step = jnp.maximum(v, 0.0) + jnp.log1p(jnp.exp(-jnp.abs(v)))
        cum = jnp.dot(
            later3[...],
            jnp.concatenate(split(step * rates[0:1], 3), axis=0),
            preferred_element_type=F32,
        )
        fall_t[m] = (cum - jnp.log(step) * LOG2E).T
        weight = jnp.exp2(cum[rows - 1 :] - cum) * step
        both = jnp.concatenate(
            [
                jnp.concatenate(split(weight, 2), axis=1),
                jnp.concatenate(split(jnp.exp2(cum), 2), axis=1),
            ],
            axis=0,
        )
        for t in range(0, pairs, 2):
            cols = slice(t * LANES, min(t + 2, pairs) * LANES)
            r = jnp.dot(both, spread_w[:, cols], preferred_element_type=F32)
            weight_x[m, :, cols] = r[:rows]
            decay_x[m, :, cols] = r[rows:]
        high, mid, last = split(cum, 3)
        last = pltpu.roll(last.astype(F32), half, 1)
        lhs_c[m] = jnp.concatenate([high, (mid.astype(F32) + last).astype(BF16)], axis=1)

    def project_gate(m):
        if m == 0:
            loads[3].wait()
        for t in range(0, pairs, 2):
            cols = slice(t * LANES, min(t + 2, pairs) * LANES)
            r = jnp.dot(ni[m], w_gate[:, cols], preferred_element_type=F32)
            gate[m, :, cols] = half_silu(0.5 * r)

    def convolve(m):
        @pl.when(place > 0)
        def _():
            rim_copy(m).wait_recv()

        def tile(t):
            taps, at = (inner_taps, t) if t < pairs else (state_taps, t - pairs)
            cols = slice(at * LANES, (at + 1) * LANES)
            total = jnp.broadcast_to(taps[reach + 1, :, cols], (rows, LANES))
            for k in range(reach + 1):
                total = total + taps[k, :, cols] * raw[m, t, pl.ds(edge - reach + k, rows), :]
            result = half_silu(total).astype(BF16)
            conv[m, t] = result
            return result

        b = tile(pairs)
        c = tile(pairs + 1)
        b_t = b.astype(F32).T.astype(BF16)
        found = lax.dot_general(c, b, (((1,), (1,)), ((), ())), preferred_element_type=F32)
        scores[m] = jnp.where(later, found, 0.0)
        for t in range(0, pairs, 2):
            end = min(t + 2, pairs)
            weighted = jnp.concatenate(
                [
                    (tile(k).astype(F32) * weight_x[m, :, k * LANES : (k + 1) * LANES]).astype(BF16)
                    for k in range(t, end)
                ],
                axis=1,
            )
            r = jnp.dot(b_t, weighted, preferred_element_type=F32)
            for k in range(t, end):
                one = r[:, (k - t) * LANES : (k - t + 1) * LANES]
                states[m, k] = one
                snd[m, k] = one.astype(BF16)

        @pl.when(place == 0)
        def _():
            for i in range(pairs):
                chain(m, i).start()

    def inside(m):
        for i in range(pairs):
            spread = jnp.dot(
                lhs_c[m],
                spread_c[:, i * pack * rows : (i + 1) * pack * rows],
                preferred_element_type=F32,
            )
            mixing = []
            for k in range(pack):
                fall = spread[:, k * rows : (k + 1) * rows] - fall_t[m, pl.ds(i * pack + k, 1), :]
                mixing.append((scores[m] * jnp.exp2(jnp.minimum(fall, CAP))).astype(BF16))
            x = conv[m, i]
            apart = [
                jnp.where(jnp.logical_and(lane >= k * head_size, lane < (k + 1) * head_size), x, 0.0)
                for k in range(pack)
            ]
            result = jnp.dot(
                jnp.concatenate(mixing, axis=1),
                jnp.concatenate([a.astype(BF16) for a in apart], axis=0),
                preferred_element_type=F32,
            )
            cols = slice(i * LANES, (i + 1) * LANES)
            base[m, :, cols] = result + skips[:, cols] * x.astype(F32)

    def scan(m):
        inside(m)
        for t in range(0, pairs, 2):
            end = min(t + 2, pairs)

            @pl.when(place > 0)
            def _():
                for i in range(t, end):
                    chain(m, i).wait_recv()

            @pl.when(jnp.logical_and(place > 0, place < n_seq - 1))
            def _():
                for i in range(t, end):
                    cols = slice(i * LANES, (i + 1) * LANES)
                    snd[m, i] = (
                        decay_x[m, rows - 1 :, cols] * ent[m, i].astype(F32) + states[m, i]
                    ).astype(BF16)
                    chain(m, i).start()

            entering = jnp.concatenate([ent[m, i] for i in range(t, end)], axis=1)
            cols = slice(t * LANES, end * LANES)
            across = jnp.dot(conv[m, pairs + 1], entering, preferred_element_type=F32)
            gated = (base[m, :, cols] + decay_x[m, :, cols] * across) * gate[m, :, cols]
            squares_of = gated * gated
            total = squares_of[:, :LANES]
            for k in range(1, end - t):
                total = total + squares_of[:, k * LANES : (k + 1) * LANES]
            sq_acc[m] += total
            g[m, :, cols] = (gated * inner_gain[:, cols]).astype(BF16)

    def project_out(m):
        if m == 0:
            loads[4].wait()
        total = jnp.sum(sq_acc[m], axis=1, keepdims=True)
        sq_own[m] = jnp.broadcast_to(total, (rows, LANES)).T[:8]
        for j in range(n_tensor):
            term[m, j] = jnp.dot(
                g[m], w_out[:, j * narrow : (j + 1) * narrow], preferred_element_type=F32
            ).astype(BF16)

            @pl.when(me != j)
            def _():
                squares(m, j).start()
                part(m, j).start()

    def finish(m):
        parts[m, me] = term[m, me]
        sq_all[m, me] = sq_own[m]
        others(lambda j: squared(m, j).wait_recv())
        others(lambda j: parted(m, j).wait_recv())
        total = sq_all[m, 0]
        for j in range(1, n_tensor):
            total = total + sq_all[m, j]
        scale = lax.rsqrt(total / (inner * n_tensor) + EPS)
        sq_acc[m] = jnp.broadcast_to(scale[0:1], (LANES, rows)).T

        def add(r, _):
            at = pl.ds(pl.multiple_of(r * 32, 32), 32)
            summed = parts[m, 0, at, :].astype(F32)
            for j in range(1, n_tensor):
                summed = summed + parts[m, j, at, :].astype(F32)
            value = (u[m, me, at, :].astype(F32) + summed * sq_acc[m, at, 0:1]).astype(BF16)
            own[m, at, :] = value
            out[0, m, at, :] = value
            return 0

        for q in range(pieces):
            lax.fori_loop(q * some // 32, (q + 1) * some // 32, add, 0)

            @pl.when(section < n_pipe - 1)
            def _():
                relay(m, q).start()

    @pl.when(section == 0)
    def _():
        hand_over(0)
        for m in range(1, micros):
            for q in range(pieces):
                send_own(m, q)
        take_input(0)
        project(0)
        project_gate(0)
        for m in range(1, micros):
            hand_over(m)
        convolve(0)
        for m in range(micros):
            if m + 1 < micros:
                take_input(m + 1)
                project(m + 1)
            if m > 0:
                finish(m - 1)
            scan(m)
            project_out(m)
            if m + 1 < micros:
                convolve(m + 1)
                project_gate(m + 1)
        finish(micros - 1)

    @pl.when(section > 0)
    def _():
        forward(0)
        hand_over(0)
        take_input(0)
        project(0)
        project_gate(0)
        convolve(0)
        for m in range(micros):
            if m + 1 < micros:
                forward(m + 1)
            if m > 0:
                finish(m - 1)
            scan(m)
            if m + 1 < micros:
                hand_over(m + 1)
            project_out(m)
            if m + 1 < micros:
                take_input(m + 1)
                project(m + 1)
                project_gate(m + 1)
                convolve(m + 1)
        finish(micros - 1)

    def drain(m, _):
        for q in range(pieces):
            near(m, q).wait_send()
            for d in range(1, chips):
                cross(m, d, q).wait_send()
                hand(m, d, q).wait_send()
        others(lambda j: part(m, j).wait_send())
        others(lambda j: squares(m, j).wait_send())

        @pl.when(place < n_seq - 1)
        def _():
            rim_copy(m).wait_send()

            def one(i, _):
                chain(m, i).wait_send()
                return 0

            lax.fori_loop(0, pairs, one, 0)

        @pl.when(section < n_pipe - 1)
        def _():
            for q in range(pieces):
                relay(m, q).wait_send()

        return 0

    lax.fori_loop(0, micros, drain, 0)


def shards(sizes, *args):
    tokens, prenorm, gate_w, inner_w, state_w, step_w = args[:6]
    n_pipe, n_tensor, n_seq = sizes
    micros, rows, narrow = tokens.shape
    width = prenorm.shape[1]
    inner = inner_w.shape[2]
    maps = state_w.shape[2]
    heads = step_w.shape[2]
    pairs = inner // LANES
    wide = inner + maps
    step_w = jnp.swapaxes(step_w, 1, 2)
    inner_taps, state_taps = (jnp.swapaxes(a, 0, 1) for a in args[6:8])
    args = (tokens, prenorm, gate_w, inner_w, state_w, step_w, inner_taps, state_taps) + args[8:]
    edge = 8
    vmem = pl.BlockSpec(memory_space=pltpu.VMEM)
    far = pl.BlockSpec(memory_space=pl.ANY)
    dma = pltpu.SemaphoreType.DMA
    V = pltpu.VMEM
    return pl.pallas_call(
        functools.partial(kernel, sizes),
        out_shape=jax.ShapeDtypeStruct((1, micros, rows, narrow), BF16),
        in_specs=[far] * len(args),
        out_specs=vmem,
        scratch_shapes=[
            V((1, width), F32),
            V(inner_taps.shape, F32),
            V(state_taps.shape, F32),
            V((1, heads), F32),
            V((1, heads), F32),
            V((1, heads), F32),
            V((1, inner), F32),
            V((width, inner), BF16),
            V((width, inner), BF16),
            V((width, maps), BF16),
            V((heads, width), BF16),
            V((inner, width), BF16),
            V((micros, n_tensor, rows, narrow), BF16),
            V((micros, rows, width), BF16),
            V((micros, wide // LANES, edge + rows, LANES), F32),
            V((micros, wide // LANES, rows, LANES), BF16),
            V((micros, rows, inner), F32),
            V((8, LANES), F32),
            V((width, LANES), BF16),
            V((rows, 3 * rows), BF16),
            V((2 * LANES, inner), BF16),
            V((2 * LANES, heads * rows), BF16),
            V((1, inner), F32),
            V((micros, rows, 2 * LANES), BF16),
            V((micros, LANES, rows), F32),
            V((micros, rows, inner), F32),
            V((micros, rows, inner), F32),
            V((micros, rows, rows), F32),
            V((micros, pairs, LANES, LANES), F32),
            V((micros, pairs, LANES, LANES), BF16),
            V((micros, pairs, LANES, LANES), BF16),
            V((micros, rows, inner), F32),
            V((micros, rows, inner), BF16),
            V((micros, rows, LANES), F32),
            V((micros, 8, rows), F32),
            V((micros, n_tensor, 8, rows), F32),
            V((micros, n_tensor, rows, narrow), BF16),
            V((micros, n_tensor, rows, narrow), BF16),
            V((micros, rows, narrow), BF16),
            dma((5,)),
            dma((7,)),
            dma((micros,)),
            dma((micros, n_tensor, 2)),
            dma((micros, n_tensor, 2)),
            dma((micros,)),
            dma((micros,)),
            dma((micros, pairs)),
            dma((micros, pairs)),
            dma((micros, n_tensor)),
            dma((micros, n_tensor)),
            dma((micros, n_tensor)),
            dma((micros, n_tensor)),
            dma((micros, 2)),
            dma((micros, 2)),
        ],
        compiler_params=pltpu.CompilerParams(
            collective_id=0, has_side_effects=True, vmem_limit_bytes=60000 * 1024
        ),
    )(*args)


def solution(mesh):
    sizes = (mesh.shape["pipe"], mesh.shape["tensor"], mesh.shape["seq"])
    placed = (
        P(None, "seq", "tensor"),
        P("pipe", None),
        P("pipe", None, "tensor"),
        P("pipe", None, "tensor"),
        P("pipe", None, None),
        P("pipe", None, "tensor"),
        P("pipe", None, "tensor"),
        P("pipe", None, None),
        P("pipe", "tensor"),
        P("pipe", "tensor"),
        P("pipe", "tensor"),
        P("pipe", "tensor"),
        P("pipe", "tensor", None),
    )
    return jax.shard_map(
        functools.partial(shards, sizes),
        mesh=mesh,
        in_specs=placed,
        out_specs=P("pipe", None, "seq", "tensor"),
        check_vma=False,
    )
```

```python
import functools

import jax
import jax.numpy as jnp
from jax import lax
from jax.experimental import pallas as pl
from jax.experimental.pallas import tpu as pltpu
from jax.sharding import PartitionSpec as P

EPS = 1e-05
LANES = 128
MESH = pl.DeviceIdType.MESH
F32 = jnp.float32
BF16 = jnp.bfloat16


LOG2E = 1.4426950408889634
CAP = 126.0


def half_silu(h):
    return h + h * jnp.tanh(h)


def split(v, parts):
    pieces = []
    for _ in range(parts - 1):
        piece = v.astype(BF16)
        pieces.append(piece)
        v = v - piece.astype(F32)
    return pieces + [v.astype(BF16)]


def remote(src, dst, send, recv, where):
    return pltpu.make_async_remote_copy(
        src_ref=src, dst_ref=dst, send_sem=send, recv_sem=recv, device_id=where, device_id_type=MESH
    )


def kernel(
    sizes,
    tokens,
    prenorm_hbm,
    gate_hbm,
    inner_hbm,
    state_hbm,
    step_hbm,
    inner_taps_hbm,
    state_taps_hbm,
    step_bias_hbm,
    decay_rate_hbm,
    skip_scale_hbm,
    inner_gain_hbm,
    out_hbm,
    out,
    prenorm,
    inner_taps,
    state_taps,
    step_bias,
    decay_rate,
    skip_scale,
    inner_gain,
    w_gate,
    w_inner,
    w_state,
    w_step,
    w_out,
    u,
    ni,
    raw,
    conv,
    gate,
    rates,
    w_step_t,
    later3,
    spread_w,
    spread_c,
    skips,
    lhs_c,
    fall_t,
    weight_x,
    decay_x,
    b_t,
    scores,
    states,
    ent,
    snd,
    base,
    g,
    sq_acc,
    sq_own,
    sq_all,
    term,
    mine,
    lent,
    bundle,
    parts,
    own,
    w_sem,
    v_sem,
    t_sem,
    ag_send,
    ag_recv,
    rim_send,
    rim_recv,
    ch_send,
    ch_recv,
    lend_send,
    lend_recv,
    rs_send,
    rs_recv,
    sq_send,
    sq_recv,
    pipe_send,
    pipe_recv,
):
    n_pipe, n_tensor, n_seq = sizes
    micros, rows, narrow = own.shape
    width = prenorm.shape[1]
    inner = w_inner.shape[1]
    heads = step_bias.shape[1]
    head_size = inner // heads
    pack = LANES // head_size
    pairs = inner // LANES
    tiles = raw.shape[1]
    reach = inner_taps.shape[0] - 2
    edge = raw.shape[2] - rows
    section = lax.axis_index("pipe")
    me = lax.axis_index("tensor")
    place = lax.axis_index("seq")
    half = LANES // 2
    wide = 2 * LANES

    core = lax.rem(me, 2)
    chip = me // 2
    partner = me + 1 - 2 * core
    chips = n_tensor // 2
    pieces = ag_send.shape[2]
    some = rows // pieces
    aligned = w_out.ndim == 3

    def chip_at(d):
        return lax.rem(chip + d, chips)

    order = list(range(1, chips)) + [0]
    lending = [(d, 2 * chip_at(d) + 1 - core) for d in order]
    keeping = [(d, 2 * chip_at(d) + core) for d in order]

    def load(src, dst, k):
        return pltpu.make_async_copy(src, dst, w_sem.at[k])

    loads = [
        load(step_hbm.at[0], w_step, 0),
        load(state_hbm.at[0], w_state, 1),
        load(inner_hbm.at[0], w_inner, 2),
        load(gate_hbm.at[0], w_gate, 3),
    ]
    if aligned:
        outs = [
            load(
                out_hbm.at[0, :, pl.ds(pl.multiple_of(j * narrow, LANES), narrow)],
                w_out.at[d, :, pl.ds(side * narrow, narrow)],
                4 + 2 * d + side,
            )
            for pair in zip(lending, keeping)
            for side, (d, j) in enumerate(pair)
        ]
    else:
        outs = [load(out_hbm.at[0], w_out, 4)]
    vectors = [
        pltpu.make_async_copy(src, dst, v_sem.at[k])
        for k, (src, dst) in enumerate(
            (
                (prenorm_hbm, prenorm),
                (inner_taps_hbm, inner_taps),
                (state_taps_hbm, state_taps),
                (step_bias_hbm, step_bias),
                (decay_rate_hbm, decay_rate),
                (skip_scale_hbm, skip_scale),
                (inner_gain_hbm, inner_gain),
            )
        )
    ]

    def stage(m):
        return pltpu.make_async_copy(tokens.at[m], u.at[m, me], t_sem.at[m])

    def at_chip(d):
        return 2 * chip_at(d) + core

    def gather(m, q, src, key, where):
        block = u.at[m, src, pl.ds(q * some, some)]
        return remote(
            block, block, ag_send.at[m, key, q], ag_recv.at[m, src, q], {"tensor": where}
        )

    def near(m, q):
        return gather(m, q, me, partner, partner)

    def cross(m, d, q):
        return gather(m, q, me, at_chip(d), at_chip(d))

    def hand(m, d, q):
        return gather(m, q, at_chip(d), at_chip(d) + 1 - 2 * core, partner)

    def gathered(m, q, src):
        return gather(m, q, src, src, partner)

    def send_own(m, q):
        for d in range(1, chips):
            cross(m, d, q).start()
        near(m, q).start()

    def rim_copy(m):
        return remote(
            raw.at[m, :, pl.ds(rows, edge)],
            raw.at[m, :, pl.ds(0, edge)],
            rim_send.at[m],
            rim_recv.at[m],
            {"seq": lax.rem(place + 1, n_seq)},
        )

    def chain(m, i):
        return remote(
            snd.at[m, i],
            ent.at[m, i],
            ch_send.at[m, i],
            ch_recv.at[m, i],
            {"seq": lax.rem(place + 1, n_seq)},
        )

    def lend(m, d, j):
        to = chip_at(d)
        return remote(
            term.at[m, j], lent.at[m, to], lend_send.at[m, d], lend_recv.at[m, to], {"tensor": partner}
        )

    def borrowed(m, d):
        to = chip_at(d)
        return remote(
            lent.at[m, to], lent.at[m, to], lend_send.at[m, d], lend_recv.at[m, to], {"tensor": partner}
        )

    def part(m, d, q):
        at = pl.ds(q * some, some)
        return remote(
            bundle.at[m, d - 1, at],
            parts.at[m, d - 1, at],
            rs_send.at[m, d - 1, q],
            rs_recv.at[m, d - 1, q],
            {"tensor": at_chip(d)},
        )

    def squares(m, j):
        return remote(
            sq_own.at[m], sq_all.at[m, me], sq_send.at[m, j], sq_recv.at[m, me], {"tensor": j}
        )

    def squared(m, j):
        return remote(
            sq_all.at[m, j], sq_all.at[m, j], sq_send.at[m, j], sq_recv.at[m, j], {"tensor": j}
        )

    def relay(m, q):
        return remote(
            own.at[m, pl.ds(q * some, some)],
            u.at[m, me, pl.ds(q * some, some)],
            pipe_send.at[m, q],
            pipe_recv.at[m, q],
            {"pipe": lax.rem(section + 1, n_pipe)},
        )

    def others(action):
        for j in range(n_tensor):
            pl.when(me != j)(functools.partial(action, j))

    @pl.when(section == 0)
    def _():
        for m in range(micros):
            stage(m).start()

    for copy in vectors + loads + outs:
        copy.start()

    barrier = pltpu.get_barrier_semaphore()

    def greet(where):
        pl.semaphore_signal(barrier, inc=1, device_id=where, device_id_type=MESH)

    others(lambda j: greet({"tensor": j}))
    partners = n_tensor - 1
    for axis, index, count in (("seq", place, n_seq), ("pipe", section, n_pipe)):
        pl.when(index > 0)(functools.partial(greet, {axis: index - 1}))
        pl.when(index < count - 1)(functools.partial(greet, {axis: index + 1}))
        partners = partners + jnp.where(index > 0, 1, 0) + jnp.where(index < count - 1, 1, 0)
    pl.semaphore_wait(barrier, partners)

    @pl.when(section == 0)
    def _():
        stage(0).wait()
        for q in range(pieces):
            send_own(0, q)

    for copy in vectors:
        copy.wait()
    inner_taps[...] = inner_taps[...] * 0.5
    state_taps[...] = state_taps[...] * 0.5
    rates[...] = jnp.zeros_like(rates)
    rates[0:1, :heads] = decay_rate[...] * (-LOG2E)
    rates[1:2, :heads] = step_bias[...]
    rates[2:3, :heads] = skip_scale[...]
    sq_acc[...] = jnp.zeros_like(sq_acc)

    @pl.when(place == 0)
    def _():
        for m in range(micros):
            raw[m, :, 0:edge, :] = jnp.zeros((tiles, edge, LANES), F32)
        ent[...] = jnp.zeros_like(ent)

    low = lax.broadcasted_iota(jnp.int32, (rows, LANES), 0)
    lane = lax.broadcasted_iota(jnp.int32, (rows, LANES), 1)
    later = low >= lane
    for k in range(3):
        later3[:, k * rows : (k + 1) * rows] = later.astype(F32).astype(BF16)

    def spreading(columns, size, first):
        k = lax.broadcasted_iota(jnp.int32, (wide, columns), 0)
        at = lax.broadcasted_iota(jnp.int32, (wide, columns), 1) + first
        row = k
        for start in (half, LANES, LANES + half):
            if size == head_size and start != LANES:
                continue
            row = jnp.where(k >= start, k - start, row)
        if size != head_size:
            row = jnp.where(jnp.logical_and(k >= half, k < LANES), LANES, row)
        inside = jnp.logical_and(at >= row * size, at < (row + 1) * size)
        return jnp.where(inside, 1.0, 0.0).astype(BF16)

    def fill_w(t, _):
        at = pl.multiple_of(t * LANES, LANES)
        spread_w[:, pl.ds(at, LANES)] = spreading(LANES, head_size, at)
        return 0

    def fill_c(t, _):
        at = pl.multiple_of(t * LANES, LANES)
        spread_c[:, pl.ds(at, LANES)] = spreading(LANES, rows, at)
        return 0

    lax.fori_loop(0, pairs, fill_w, 0)
    lax.fori_loop(0, heads, fill_c, 0)
    for t in range(pairs):
        cols = slice(t * LANES, (t + 1) * LANES)
        r = lax.broadcasted_iota(jnp.int32, (8, LANES), 0)
        whole = jnp.broadcast_to(rates[2:3], (8, LANES))
        h0 = lax.broadcasted_iota(jnp.int32, (8, LANES), 1)
        row = jnp.zeros((8, LANES), F32)
        for k in range(pack):
            one = jnp.sum(jnp.where(h0 == t * pack + k, whole, 0.0), axis=1, keepdims=True)
            row = jnp.where(h0 >= k * head_size, one, row)
        skips[:, cols] = row[0:1]

    loads[0].wait()
    w_step_t[...] = (
        jnp.concatenate([w_step[...].astype(F32), jnp.zeros((LANES - heads, width), F32)], axis=0)
        .T.astype(BF16)
    )

    def forward(m):
        for q in range(pieces):
            relay(m, q).wait_recv()
            send_own(m, q)

    def hand_over(m):
        for q in range(pieces):
            for d in range(1, chips):
                gathered(m, q, at_chip(d)).wait_recv()
                hand(m, d, q).start()

    def take_input(m):
        for q in range(pieces):
            gathered(m, q, partner).wait_recv()
            for d in range(1, chips):
                gathered(m, q, at_chip(d) + 1 - 2 * core).wait_recv()
            at = slice(q * some, (q + 1) * some)
            total = jnp.zeros((some, 1), F32)
            for j in range(n_tensor):
                v = u[m, j, at, :].astype(F32)
                total = total + jnp.sum(v * v, axis=1, keepdims=True)
            scale = lax.rsqrt(total / width + EPS)
            for j in range(n_tensor):
                cols = slice(j * narrow, (j + 1) * narrow)
                v = u[m, j, at, :].astype(F32)
                ni[m, at, cols] = (v * scale * prenorm[:, cols]).astype(BF16)

    def multiply(m, first, begin, end, weights):
        for t in range(begin, end, 2):
            stop = min(t + 2, end)
            r = jnp.dot(ni[m], weights[:, t * LANES : stop * LANES], preferred_element_type=F32)
            for k in range(t, stop):
                raw[m, first + k, edge:, :] = r[:, (k - t) * LANES : (k - t + 1) * LANES]

    def send_rim(m):
        @pl.when(place < n_seq - 1)
        def _():
            rim_copy(m).start()

    def step_sizes(m):
        v = jnp.dot(ni[m], w_step_t[...], preferred_element_type=F32) + rates[1:2]
        step = jnp.maximum(v, 0.0) + jnp.log1p(jnp.exp(-jnp.abs(v)))
        cum = jnp.dot(
            later3[...],
            jnp.concatenate(split(step * rates[0:1], 3), axis=0),
            preferred_element_type=F32,
        )
        fall_t[m] = (cum - jnp.log(step) * LOG2E).T
        weight = jnp.exp2(cum[rows - 1 :] - cum) * step
        both = jnp.concatenate(
            [
                jnp.concatenate(split(weight, 2), axis=1),
                jnp.concatenate(split(jnp.exp2(cum), 2), axis=1),
            ],
            axis=0,
        )
        for t in range(0, pairs, 2):
            cols = slice(t * LANES, min(t + 2, pairs) * LANES)
            r = jnp.dot(both, spread_w[:, cols], preferred_element_type=F32)
            weight_x[m, :, cols] = r[:rows]
            decay_x[m, :, cols] = r[rows:]
        high, mid, last = split(cum, 3)
        last = pltpu.roll(last.astype(F32), half, 1)
        lhs_c[m] = jnp.concatenate([high, (mid.astype(F32) + last).astype(BF16)], axis=1)

    def project(m):
        if m == 0:
            loads[1].wait()
            loads[2].wait()
        step_sizes(m)
        multiply(m, pairs, 0, tiles - pairs, w_state)
        multiply(m, 0, 0, pairs, w_inner)
        send_rim(m)

    def gate_some(m, begin, end):
        for t in range(begin, end, 2):
            cols = slice(t * LANES, min(t + 2, end) * LANES)
            r = jnp.dot(ni[m], w_gate[:, cols], preferred_element_type=F32)
            gate[m, :, cols] = half_silu(0.5 * r)

    def project_gate(m):
        if m == 0:
            loads[3].wait()
        gate_some(m, 0, pairs)

    def tile(m, t):
        taps, at = (inner_taps, t) if t < pairs else (state_taps, t - pairs)
        cols = slice(at * LANES, (at + 1) * LANES)
        total = jnp.broadcast_to(taps[reach + 1, :, cols], (rows, LANES))
        for k in range(reach + 1):
            total = total + taps[k, :, cols] * raw[m, t, pl.ds(edge - reach + k, rows), :]
        result = half_silu(total).astype(BF16)
        conv[m, t] = result
        return result

    def convolve_maps(m):
        @pl.when(place > 0)
        def _():
            rim_copy(m).wait_recv()

        b = tile(m, pairs)
        c = tile(m, pairs + 1)
        b_t[m] = b.astype(F32).T.astype(BF16)
        found = lax.dot_general(c, b, (((1,), (1,)), ((), ())), preferred_element_type=F32)
        scores[m] = jnp.where(later, found, 0.0)

    def convolve_some(m, begin, end):
        for t in range(begin, end, 2):
            stop = min(t + 2, end)
            weighted = jnp.concatenate(
                [
                    (
                        tile(m, k).astype(F32) * weight_x[m, :, k * LANES : (k + 1) * LANES]
                    ).astype(BF16)
                    for k in range(t, stop)
                ],
                axis=1,
            )
            r = jnp.dot(b_t[m], weighted, preferred_element_type=F32)
            for k in range(t, stop):
                one = r[:, (k - t) * LANES : (k - t + 1) * LANES]
                states[m, k] = one
                snd[m, k] = one.astype(BF16)

        @pl.when(place == 0)
        def _():
            for i in range(begin, end):
                chain(m, i).start()

    middle = pairs // 4 * 2

    def convolve(m):
        convolve_maps(m)
        convolve_some(m, 0, middle)
        convolve_some(m, middle, pairs)

    def inside_some(m, begin, end):
        for i in range(begin, end):
            spread = jnp.dot(
                lhs_c[m],
                spread_c[:, i * pack * rows : (i + 1) * pack * rows],
                preferred_element_type=F32,
            )
            mixing = []
            for k in range(pack):
                fall = spread[:, k * rows : (k + 1) * rows] - fall_t[m, pl.ds(i * pack + k, 1), :]
                mixing.append((scores[m] * jnp.exp2(jnp.minimum(fall, CAP))).astype(BF16))
            x = conv[m, i]
            apart = [
                jnp.where(jnp.logical_and(lane >= k * head_size, lane < (k + 1) * head_size), x, 0.0)
                for k in range(pack)
            ]
            result = jnp.dot(
                jnp.concatenate(mixing, axis=1),
                jnp.concatenate([a.astype(BF16) for a in apart], axis=0),
                preferred_element_type=F32,
            )
            cols = slice(i * LANES, (i + 1) * LANES)
            base[m, :, cols] = result + skips[:, cols] * x.astype(F32)

    def inside(m):
        inside_some(m, 0, pairs)

    def poll(m, i):
        @pl.when(place > 0)
        def _():
            chain(m, i).wait_recv()

        @pl.when(jnp.logical_and(place > 0, place < n_seq - 1))
        def _():
            cols = slice(i * LANES, (i + 1) * LANES)
            snd[m, i] = (
                decay_x[m, rows - 1 :, cols] * ent[m, i].astype(F32) + states[m, i]
            ).astype(BF16)
            chain(m, i).start()

    def across(m, t, end):
        entering = jnp.concatenate([ent[m, i] for i in range(t, end)], axis=1)
        cols = slice(t * LANES, end * LANES)
        over = jnp.dot(conv[m, pairs + 1], entering, preferred_element_type=F32)
        gated = (base[m, :, cols] + decay_x[m, :, cols] * over) * gate[m, :, cols]
        squares_of = gated * gated
        total = squares_of[:, :LANES]
        for k in range(1, end - t):
            total = total + squares_of[:, k * LANES : (k + 1) * LANES]
        sq_acc[m] += total
        g[m, :, cols] = (gated * inner_gain[:, cols]).astype(BF16)

    def scan(m, between=()):
        between = dict(between)
        for t in range(0, pairs, 2):
            end = min(t + 2, pairs)
            for i in range(t, end):
                poll(m, i)
                if i in between and i < end - 1:
                    between[i]()
            across(m, t, end)
            if end - 1 in between:
                between[end - 1]()

    def project_out(m):
        if m == 0:
            for copy in outs:
                copy.wait()
        if aligned:
            for d, j in lending:
                r = jnp.dot(g[m], w_out[d], preferred_element_type=F32)
                term[m, j] = r[:, :narrow].astype(BF16)
                lend(m, d, j).start()
                mine[m, d] = r[:, narrow:]
        else:
            for j in range(n_tensor):
                r = jnp.dot(
                    g[m], w_out[:, j * narrow : (j + 1) * narrow], preferred_element_type=F32
                )
                d = lax.rem(j // 2 - chip + chips, chips)
                term[m, j] = r.astype(BF16)
                mine[m, d] = jnp.where(core == j % 2, r, mine[m, d])
            for d, j in lending:
                lend(m, d, j).start()
        total = jnp.sum(sq_acc[m], axis=1, keepdims=True)
        sq_own[m] = jnp.broadcast_to(total, (rows, LANES)).T[:8]
        others(lambda j: squares(m, j).start())

    def combine(m):
        for d in range(1, chips):
            borrowed(m, d).wait_recv()
            for q in range(pieces):
                at = slice(q * some, (q + 1) * some)
                bundle[m, d - 1, at, :] = (
                    mine[m, d, at, :] + lent[m, chip_at(d), at, :].astype(F32)
                ).astype(BF16)
                part(m, d, q).start()

    def finish(m):
        sq_all[m, me] = sq_own[m]
        others(lambda j: squared(m, j).wait_recv())
        total = sq_all[m, 0]
        for j in range(1, n_tensor):
            total = total + sq_all[m, j]
        scale = lax.rsqrt(total / (inner * n_tensor) + EPS)
        sq_acc[m] = jnp.broadcast_to(scale[0:1], (LANES, rows)).T
        borrowed(m, 0).wait_recv()
        for q in range(pieces):
            at = slice(q * some, (q + 1) * some)
            for d in range(1, chips):
                part(m, d, q).wait_recv()
            summed = mine[m, 0, at, :] + lent[m, chip, at, :].astype(F32)
            for d in range(1, chips):
                summed = summed + parts[m, d - 1, at, :].astype(F32)
            value = (u[m, me, at, :].astype(F32) + summed * sq_acc[m, at, 0:1]).astype(BF16)
            own[m, at, :] = value
            out[0, m, at, :] = value

            @pl.when(section < n_pipe - 1)
            def _():
                relay(m, q).start()

    first = section == 0
    weave = jnp.logical_and(first, place > 0)

    def next_input(m):
        for q in range(pieces):
            send_own(m, q)

    @pl.when(first)
    def _():
        hand_over(0)
        for m in range(1, micros):
            stage(m).wait()
            next_input(m)

    @pl.when(section > 0)
    def _():
        forward(0)
        hand_over(0)

    take_input(0)
    project(0)
    pl.when(place == 0)(lambda: convolve(0))
    project_gate(0)
    pl.when(place > 0)(lambda: convolve(0))

    @pl.when(section > 0)
    def _():
        for m in range(1, micros):
            forward(m)

    inside(0)

    @pl.when(first)
    def _():
        for m in range(1, micros):
            hand_over(m)

    for m in range(1, micros):

        @pl.when(weave)
        def _():
            take_input(m)
            count = tiles - pairs
            third = pairs // 3 // 2 * 2 + 2
            work = [
                lambda: multiply(m, pairs, 0, count, w_state),
                lambda: multiply(m, 0, 0, third, w_inner),
                lambda: (multiply(m, 0, third, pairs, w_inner), send_rim(m)),
                lambda: step_sizes(m),
                lambda: gate_some(m, 0, third),
                lambda: gate_some(m, third, pairs),
                lambda: (convolve_maps(m), convolve_some(m, 0, middle)),
                lambda: convolve_some(m, middle, pairs),
                lambda: inside_some(m, 0, pairs // 2),
                lambda: inside_some(m, pairs // 2, pairs),
            ]
            between = {}
            for k, step in enumerate(work):
                between.setdefault(k * pairs // len(work), []).append(step)
            scan(
                m - 1,
                {
                    k: (lambda steps=steps: [step() for step in steps])
                    for k, steps in between.items()
                },
            )
            project_out(m - 1)
            combine(m - 1)

        @pl.when(section > 0)
        def _():
            scan(
                m - 1,
                {pairs // 2 - 1: lambda: (hand_over(m), take_input(m), project(m), project_gate(m))},
            )
            convolve(m)
            inside(m)

        @pl.when(jnp.logical_and(first, place == 0))
        def _():
            scan(m - 1)
            project_out(m - 1)
            combine(m - 1)
            take_input(m)
            project(m)
            convolve(m)
            project_gate(m)
            inside(m)
            finish(m - 1)

        def early():
            pl.when(section > 0)(lambda: project_out(m - 1))

        def late():
            pl.when(weave)(lambda: finish(m - 1))
            pl.when(section > 0)(lambda: combine(m - 1))

        scan(m, {0: early, pairs * 7 // 10: late})

    project_out(micros - 1)
    combine(micros - 1)

    @pl.when(section > 0)
    def _():
        for m in range(micros - 1):
            finish(m)

    finish(micros - 1)

    def drain(m, _):
        for q in range(pieces):
            near(m, q).wait_send()
            for d in range(1, chips):
                cross(m, d, q).wait_send()
                hand(m, d, q).wait_send()
        for d, j in lending:
            lend(m, d, j).wait_send()
        for q in range(pieces):
            for d in range(1, chips):
                part(m, d, q).wait_send()
        others(lambda j: squares(m, j).wait_send())

        @pl.when(place < n_seq - 1)
        def _():
            rim_copy(m).wait_send()

            def one(i, _):
                chain(m, i).wait_send()
                return 0

            lax.fori_loop(0, pairs, one, 0)

        @pl.when(section < n_pipe - 1)
        def _():
            for q in range(pieces):
                relay(m, q).wait_send()

        return 0

    lax.fori_loop(0, micros, drain, 0)


def shards(sizes, *args):
    tokens, prenorm, gate_w, inner_w, state_w, step_w = args[:6]
    n_pipe, n_tensor, n_seq = sizes
    micros, rows, narrow = tokens.shape
    width = prenorm.shape[1]
    inner = inner_w.shape[2]
    maps = state_w.shape[2]
    heads = step_w.shape[2]
    pairs = inner // LANES
    wide = inner + maps
    step_w = jnp.swapaxes(step_w, 1, 2)
    inner_taps, state_taps = (jnp.swapaxes(a, 0, 1) for a in args[6:8])
    args = (tokens, prenorm, gate_w, inner_w, state_w, step_w, inner_taps, state_taps) + args[8:]
    edge = 8
    chips = n_tensor // 2
    pieces = 4
    vmem = pl.BlockSpec(memory_space=pltpu.VMEM)
    far = pl.BlockSpec(memory_space=pltpu.HBM)
    dma = pltpu.SemaphoreType.DMA
    V = pltpu.VMEM
    return pl.pallas_call(
        functools.partial(kernel, sizes),
        out_shape=pltpu.VMEM((1, micros, rows, narrow), BF16),
        in_specs=[far] * len(args),
        out_specs=vmem,
        scratch_shapes=[
            V((1, width), F32),
            V(inner_taps.shape, F32),
            V(state_taps.shape, F32),
            V((1, heads), F32),
            V((1, heads), F32),
            V((1, heads), F32),
            V((1, inner), F32),
            V((width, inner), BF16),
            V((width, inner), BF16),
            V((width, maps), BF16),
            V((heads, width), BF16),
            V((chips, inner, 2 * narrow) if narrow % LANES == 0 else (inner, width), BF16),
            V((micros, n_tensor, rows, narrow), BF16),
            V((micros, rows, width), BF16),
            V((micros, wide // LANES, edge + rows, LANES), F32),
            V((micros, wide // LANES, rows, LANES), BF16),
            V((micros, rows, inner), F32),
            V((8, LANES), F32),
            V((width, LANES), BF16),
            V((rows, 3 * rows), BF16),
            V((2 * LANES, inner), BF16),
            V((2 * LANES, heads * rows), BF16),
            V((1, inner), F32),
            V((micros, rows, 2 * LANES), BF16),
            V((micros, LANES, rows), F32),
            V((micros, rows, inner), F32),
            V((micros, rows, inner), F32),
            V((micros, LANES, rows), BF16),
            V((micros, rows, rows), F32),
            V((micros, pairs, LANES, LANES), F32),
            V((micros, pairs, LANES, LANES), BF16),
            V((micros, pairs, LANES, LANES), BF16),
            V((micros, rows, inner), F32),
            V((micros, rows, inner), BF16),
            V((micros, rows, LANES), F32),
            V((micros, 8, rows), F32),
            V((micros, n_tensor, 8, rows), F32),
            V((micros, n_tensor, rows, narrow), BF16),
            V((micros, chips, rows, narrow), F32),
            V((micros, chips, rows, narrow), BF16),
            V((micros, chips - 1, rows, narrow), BF16),
            V((micros, chips - 1, rows, narrow), BF16),
            V((micros, rows, narrow), BF16),
            dma((4 + n_tensor,)),
            dma((7,)),
            dma((micros,)),
            dma((micros, n_tensor, pieces)),
            dma((micros, n_tensor, pieces)),
            dma((micros,)),
            dma((micros,)),
            dma((micros, pairs)),
            dma((micros, pairs)),
            dma((micros, chips)),
            dma((micros, chips)),
            dma((micros, chips - 1, pieces)),
            dma((micros, chips - 1, pieces)),
            dma((micros, n_tensor)),
            dma((micros, n_tensor)),
            dma((micros, pieces)),
            dma((micros, pieces)),
        ],
        compiler_params=pltpu.CompilerParams(
            collective_id=0, has_side_effects=True, vmem_limit_bytes=60000 * 1024
        ),
    )(*args)


def solution(mesh):
    sizes = (mesh.shape["pipe"], mesh.shape["tensor"], mesh.shape["seq"])
    placed = (
        P(None, "seq", "tensor"),
        P("pipe", None),
        P("pipe", None, "tensor"),
        P("pipe", None, "tensor"),
        P("pipe", None, None),
        P("pipe", None, "tensor"),
        P("pipe", None, "tensor"),
        P("pipe", None, None),
        P("pipe", "tensor"),
        P("pipe", "tensor"),
        P("pipe", "tensor"),
        P("pipe", "tensor"),
        P("pipe", "tensor", None),
    )
    return jax.shard_map(
        functools.partial(shards, sizes),
        mesh=mesh,
        in_specs=placed,
        out_specs=P("pipe", None, "seq", "tensor"),
        check_vma=False,
    )
```

```python
import functools

import jax
import jax.numpy as jnp
from jax import lax
from jax.experimental import pallas as pl
from jax.experimental.pallas import tpu as pltpu
from jax.sharding import PartitionSpec as P

EPS = 1e-05
LANES = 128
MESH = pl.DeviceIdType.MESH
F32 = jnp.float32
BF16 = jnp.bfloat16


LOG2E = 1.4426950408889634
CAP = 126.0


def half_silu(h):
    return h + h * jnp.tanh(h)


def split(v, parts):
    pieces = []
    for _ in range(parts - 1):
        piece = v.astype(BF16)
        pieces.append(piece)
        v = v - piece.astype(F32)
    return pieces + [v.astype(BF16)]


def remote(src, dst, send, recv, where):
    return pltpu.make_async_remote_copy(
        src_ref=src, dst_ref=dst, send_sem=send, recv_sem=recv, device_id=where, device_id_type=MESH
    )


def kernel(
    sizes,
    tokens,
    prenorm_hbm,
    gate_hbm,
    inner_hbm,
    state_hbm,
    step_hbm,
    inner_taps_hbm,
    state_taps_hbm,
    step_bias_hbm,
    decay_rate_hbm,
    skip_scale_hbm,
    inner_gain_hbm,
    out_hbm,
    out,
    prenorm,
    inner_taps,
    state_taps,
    step_bias,
    decay_rate,
    skip_scale,
    inner_gain,
    w_gate,
    w_inner,
    w_state,
    w_step,
    w_out,
    u,
    ni,
    raw,
    conv,
    gate,
    rates,
    w_step_t,
    later3,
    spread_w,
    spread_c,
    skips,
    lhs_c,
    fall_t,
    weight_x,
    decay_x,
    b_t,
    scores,
    states,
    ent,
    snd,
    base,
    g,
    sq_acc,
    sq_own,
    sq_all,
    term,
    mine,
    lent,
    bundle,
    parts,
    own,
    w_sem,
    v_sem,
    t_sem,
    ag_send,
    ag_recv,
    rim_send,
    rim_recv,
    ch_send,
    ch_recv,
    lend_send,
    lend_recv,
    rs_send,
    rs_recv,
    sq_send,
    sq_recv,
    pipe_send,
    pipe_recv,
):
    n_pipe, n_tensor, n_seq = sizes
    micros, rows, narrow = own.shape
    width = prenorm.shape[1]
    inner = w_inner.shape[1]
    heads = step_bias.shape[1]
    head_size = inner // heads
    pack = LANES // head_size
    pairs = inner // LANES
    tiles = raw.shape[1]
    reach = inner_taps.shape[0] - 2
    edge = raw.shape[2] - rows
    section = lax.axis_index("pipe")
    me = lax.axis_index("tensor")
    place = lax.axis_index("seq")
    half = LANES // 2
    wide = 2 * LANES

    core = lax.rem(me, 2)
    chip = me // 2
    partner = me + 1 - 2 * core
    chips = n_tensor // 2
    pieces = ag_send.shape[2]
    some = rows // pieces
    aligned = w_out.ndim == 3

    def chip_at(d):
        return lax.rem(chip + d, chips)

    order = list(range(1, chips)) + [0]
    lending = [(d, 2 * chip_at(d) + 1 - core) for d in order]
    keeping = [(d, 2 * chip_at(d) + core) for d in order]

    def load(src, dst, k):
        return pltpu.make_async_copy(src, dst, w_sem.at[k])

    loads = [
        load(step_hbm.at[0], w_step, 0),
        load(state_hbm.at[0], w_state, 1),
        load(inner_hbm.at[0], w_inner, 2),
        load(gate_hbm.at[0], w_gate, 3),
    ]
    if aligned:
        outs = [
            load(
                out_hbm.at[0, :, pl.ds(pl.multiple_of(j * narrow, LANES), narrow)],
                w_out.at[d, :, pl.ds(side * narrow, narrow)],
                4 + 2 * d + side,
            )
            for pair in zip(lending, keeping)
            for side, (d, j) in enumerate(pair)
        ]
    else:
        outs = [load(out_hbm.at[0], w_out, 4)]
    vectors = [
        pltpu.make_async_copy(src, dst, v_sem.at[k])
        for k, (src, dst) in enumerate(
            (
                (prenorm_hbm, prenorm),
                (inner_taps_hbm, inner_taps),
                (state_taps_hbm, state_taps),
                (step_bias_hbm, step_bias),
                (decay_rate_hbm, decay_rate),
                (skip_scale_hbm, skip_scale),
                (inner_gain_hbm, inner_gain),
            )
        )
    ]

    def stage(m):
        return pltpu.make_async_copy(tokens.at[m], u.at[m, me], t_sem.at[m])

    def at_chip(d):
        return 2 * chip_at(d) + core

    def gather(m, q, src, key, where):
        block = u.at[m, src, pl.ds(q * some, some)]
        return remote(
            block, block, ag_send.at[m, key, q], ag_recv.at[m, src, q], {"tensor": where}
        )

    def near(m, q):
        return gather(m, q, me, partner, partner)

    def cross(m, d, q):
        return gather(m, q, me, at_chip(d), at_chip(d))

    def hand(m, d, q):
        return gather(m, q, at_chip(d), at_chip(d) + 1 - 2 * core, partner)

    def gathered(m, q, src):
        return gather(m, q, src, src, partner)

    def send_own(m, q):
        for d in range(1, chips):
            cross(m, d, q).start()
        near(m, q).start()

    def rim_copy(m):
        return remote(
            raw.at[m, :, pl.ds(rows, edge)],
            raw.at[m, :, pl.ds(0, edge)],
            rim_send.at[m],
            rim_recv.at[m],
            {"seq": lax.rem(place + 1, n_seq)},
        )

    def chain(m, i):
        return remote(
            snd.at[m, i],
            ent.at[m, i],
            ch_send.at[m, i],
            ch_recv.at[m, i],
            {"seq": lax.rem(place + 1, n_seq)},
        )

    def lend(m, d, j):
        to = chip_at(d)
        return remote(
            term.at[m, j], lent.at[m, to], lend_send.at[m, d], lend_recv.at[m, to], {"tensor": partner}
        )

    def borrowed(m, d):
        to = chip_at(d)
        return remote(
            lent.at[m, to], lent.at[m, to], lend_send.at[m, d], lend_recv.at[m, to], {"tensor": partner}
        )

    def part(m, d, q):
        at = pl.ds(q * some, some)
        return remote(
            bundle.at[m, d - 1, at],
            parts.at[m, d - 1, at],
            rs_send.at[m, d - 1, q],
            rs_recv.at[m, d - 1, q],
            {"tensor": at_chip(d)},
        )

    def squares(m, j):
        return remote(
            sq_own.at[m], sq_all.at[m, me], sq_send.at[m, j], sq_recv.at[m, me], {"tensor": j}
        )

    def squared(m, j):
        return remote(
            sq_all.at[m, j], sq_all.at[m, j], sq_send.at[m, j], sq_recv.at[m, j], {"tensor": j}
        )

    def relay(m, q):
        return remote(
            own.at[m, pl.ds(q * some, some)],
            u.at[m, me, pl.ds(q * some, some)],
            pipe_send.at[m, q],
            pipe_recv.at[m, q],
            {"pipe": lax.rem(section + 1, n_pipe)},
        )

    def others(action):
        for j in range(n_tensor):
            pl.when(me != j)(functools.partial(action, j))

    @pl.when(section == 0)
    def _():
        stage(0).start()

    for copy in vectors + loads[:1]:
        copy.start()

    barrier = pltpu.get_barrier_semaphore()

    def greet(where):
        pl.semaphore_signal(barrier, inc=1, device_id=where, device_id_type=MESH)

    others(lambda j: greet({"tensor": j}))
    partners = n_tensor - 1
    for axis, index, count in (("seq", place, n_seq), ("pipe", section, n_pipe)):
        pl.when(index > 0)(functools.partial(greet, {axis: index - 1}))
        pl.when(index < count - 1)(functools.partial(greet, {axis: index + 1}))
        partners = partners + jnp.where(index > 0, 1, 0) + jnp.where(index < count - 1, 1, 0)
    pl.semaphore_wait(barrier, partners)

    @pl.when(section == 0)
    def _():
        stage(0).wait()
        for q in range(pieces):
            send_own(0, q)

    for copy in loads[1:]:
        copy.start()

    @pl.when(section == 0)
    def _():
        for m in range(1, micros):
            stage(m).start()

    for copy in outs:
        copy.start()
    for copy in vectors:
        copy.wait()
    inner_taps[...] = inner_taps[...] * 0.5
    state_taps[...] = state_taps[...] * 0.5
    rates[...] = jnp.zeros_like(rates)
    rates[0:1, :heads] = decay_rate[...] * (-LOG2E)
    rates[1:2, :heads] = step_bias[...]
    rates[2:3, :heads] = skip_scale[...]
    sq_acc[...] = jnp.zeros_like(sq_acc)

    @pl.when(place == 0)
    def _():
        for m in range(micros):
            raw[m, :, 0:edge, :] = jnp.zeros((tiles, edge, LANES), F32)
        ent[...] = jnp.zeros_like(ent)

    low = lax.broadcasted_iota(jnp.int32, (rows, LANES), 0)
    lane = lax.broadcasted_iota(jnp.int32, (rows, LANES), 1)
    later = low >= lane
    for k in range(3):
        later3[:, k * rows : (k + 1) * rows] = later.astype(F32).astype(BF16)

    def spreading(columns, size, first):
        k = lax.broadcasted_iota(jnp.int32, (wide, columns), 0)
        at = lax.broadcasted_iota(jnp.int32, (wide, columns), 1) + first
        row = k
        for start in (half, LANES, LANES + half):
            if size == head_size and start != LANES:
                continue
            row = jnp.where(k >= start, k - start, row)
        if size != head_size:
            row = jnp.where(jnp.logical_and(k >= half, k < LANES), LANES, row)
        inside = jnp.logical_and(at >= row * size, at < (row + 1) * size)
        return jnp.where(inside, 1.0, 0.0).astype(BF16)

    def fill_w(t, _):
        at = pl.multiple_of(t * LANES, LANES)
        spread_w[:, pl.ds(at, LANES)] = spreading(LANES, head_size, at)
        return 0

    def fill_c(t, _):
        at = pl.multiple_of(t * LANES, LANES)
        spread_c[:, pl.ds(at, LANES)] = spreading(LANES, rows, at)
        return 0

    lax.fori_loop(0, pairs, fill_w, 0)
    lax.fori_loop(0, heads, fill_c, 0)
    for t in range(pairs):
        cols = slice(t * LANES, (t + 1) * LANES)
        r = lax.broadcasted_iota(jnp.int32, (8, LANES), 0)
        whole = jnp.broadcast_to(rates[2:3], (8, LANES))
        h0 = lax.broadcasted_iota(jnp.int32, (8, LANES), 1)
        row = jnp.zeros((8, LANES), F32)
        for k in range(pack):
            one = jnp.sum(jnp.where(h0 == t * pack + k, whole, 0.0), axis=1, keepdims=True)
            row = jnp.where(h0 >= k * head_size, one, row)
        skips[:, cols] = row[0:1]

    loads[0].wait()
    w_step_t[...] = (
        jnp.concatenate([w_step[...].astype(F32), jnp.zeros((LANES - heads, width), F32)], axis=0)
        .T.astype(BF16)
    )

    def forward(m):
        for q in range(pieces):
            relay(m, q).wait_recv()
            send_own(m, q)

    def hand_over(m):
        for q in range(pieces):
            for d in range(1, chips):
                gathered(m, q, at_chip(d)).wait_recv()
                hand(m, d, q).start()

    def take_input(m):
        for q in range(pieces):
            gathered(m, q, partner).wait_recv()
            for d in range(1, chips):
                gathered(m, q, at_chip(d) + 1 - 2 * core).wait_recv()
            at = slice(q * some, (q + 1) * some)
            total = jnp.zeros((some, 1), F32)
            for j in range(n_tensor):
                v = u[m, j, at, :].astype(F32)
                total = total + jnp.sum(v * v, axis=1, keepdims=True)
            scale = lax.rsqrt(total / width + EPS)
            for j in range(n_tensor):
                cols = slice(j * narrow, (j + 1) * narrow)
                v = u[m, j, at, :].astype(F32)
                ni[m, at, cols] = (v * scale * prenorm[:, cols]).astype(BF16)

    def multiply(m, first, begin, end, weights):
        for t in range(begin, end, 2):
            stop = min(t + 2, end)
            r = jnp.dot(ni[m], weights[:, t * LANES : stop * LANES], preferred_element_type=F32)
            for k in range(t, stop):
                raw[m, first + k, edge:, :] = r[:, (k - t) * LANES : (k - t + 1) * LANES]

    def send_rim(m):
        @pl.when(place < n_seq - 1)
        def _():
            rim_copy(m).start()

    def step_sizes(m):
        v = jnp.dot(ni[m], w_step_t[...], preferred_element_type=F32) + rates[1:2]
        step = jnp.maximum(v, 0.0) + jnp.log1p(jnp.exp(-jnp.abs(v)))
        cum = jnp.dot(
            later3[...],
            jnp.concatenate(split(step * rates[0:1], 3), axis=0),
            preferred_element_type=F32,
        )
        fall_t[m] = (cum - jnp.log(step) * LOG2E).T
        weight = jnp.exp2(cum[rows - 1 :] - cum) * step
        both = jnp.concatenate(
            [
                jnp.concatenate(split(weight, 2), axis=1),
                jnp.concatenate(split(jnp.exp2(cum), 2), axis=1),
            ],
            axis=0,
        )
        for t in range(0, pairs, 2):
            cols = slice(t * LANES, min(t + 2, pairs) * LANES)
            r = jnp.dot(both, spread_w[:, cols], preferred_element_type=F32)
            weight_x[m, :, cols] = r[:rows]
            decay_x[m, :, cols] = r[rows:]
        high, mid, last = split(cum, 3)
        last = pltpu.roll(last.astype(F32), half, 1)
        lhs_c[m] = jnp.concatenate([high, (mid.astype(F32) + last).astype(BF16)], axis=1)

    def project(m):
        if m == 0:
            loads[1].wait()
            loads[2].wait()
        step_sizes(m)
        multiply(m, pairs, 0, tiles - pairs, w_state)
        multiply(m, 0, 0, pairs, w_inner)
        send_rim(m)

    def gate_some(m, begin, end):
        for t in range(begin, end, 2):
            cols = slice(t * LANES, min(t + 2, end) * LANES)
            r = jnp.dot(ni[m], w_gate[:, cols], preferred_element_type=F32)
            gate[m, :, cols] = half_silu(0.5 * r)

    def project_gate(m):
        if m == 0:
            loads[3].wait()
        gate_some(m, 0, pairs)

    def tile(m, t):
        taps, at = (inner_taps, t) if t < pairs else (state_taps, t - pairs)
        cols = slice(at * LANES, (at + 1) * LANES)
        total = jnp.broadcast_to(taps[reach + 1, :, cols], (rows, LANES))
        for k in range(reach + 1):
            total = total + taps[k, :, cols] * raw[m, t, pl.ds(edge - reach + k, rows), :]
        result = half_silu(total).astype(BF16)
        conv[m, t] = result
        return result

    def convolve_maps(m):
        @pl.when(place > 0)
        def _():
            rim_copy(m).wait_recv()

        b = tile(m, pairs)
        c = tile(m, pairs + 1)
        b_t[m] = b.astype(F32).T.astype(BF16)
        found = lax.dot_general(c, b, (((1,), (1,)), ((), ())), preferred_element_type=F32)
        scores[m] = jnp.where(later, found, 0.0)

    def convolve_some(m, begin, end):
        for t in range(begin, end, 2):
            stop = min(t + 2, end)
            weighted = jnp.concatenate(
                [
                    (
                        tile(m, k).astype(F32) * weight_x[m, :, k * LANES : (k + 1) * LANES]
                    ).astype(BF16)
                    for k in range(t, stop)
                ],
                axis=1,
            )
            r = jnp.dot(b_t[m], weighted, preferred_element_type=F32)
            for k in range(t, stop):
                one = r[:, (k - t) * LANES : (k - t + 1) * LANES]
                states[m, k] = one
                snd[m, k] = one.astype(BF16)

        @pl.when(place == 0)
        def _():
            for i in range(begin, end):
                chain(m, i).start()

    middle = pairs // 4 * 2

    def convolve(m):
        convolve_maps(m)
        convolve_some(m, 0, middle)
        convolve_some(m, middle, pairs)

    def inside_some(m, begin, end):
        for i in range(begin, end):
            spread = jnp.dot(
                lhs_c[m],
                spread_c[:, i * pack * rows : (i + 1) * pack * rows],
                preferred_element_type=F32,
            )
            mixing = []
            for k in range(pack):
                fall = spread[:, k * rows : (k + 1) * rows] - fall_t[m, pl.ds(i * pack + k, 1), :]
                mixing.append((scores[m] * jnp.exp2(jnp.minimum(fall, CAP))).astype(BF16))
            x = conv[m, i]
            apart = [
                jnp.where(jnp.logical_and(lane >= k * head_size, lane < (k + 1) * head_size), x, 0.0)
                for k in range(pack)
            ]
            result = jnp.dot(
                jnp.concatenate(mixing, axis=1),
                jnp.concatenate([a.astype(BF16) for a in apart], axis=0),
                preferred_element_type=F32,
            )
            cols = slice(i * LANES, (i + 1) * LANES)
            base[m, :, cols] = result + skips[:, cols] * x.astype(F32)

    def inside(m):
        inside_some(m, 0, pairs)

    def poll(m, i):
        @pl.when(place > 0)
        def _():
            chain(m, i).wait_recv()

        @pl.when(jnp.logical_and(place > 0, place < n_seq - 1))
        def _():
            cols = slice(i * LANES, (i + 1) * LANES)
            snd[m, i] = (
                decay_x[m, rows - 1 :, cols] * ent[m, i].astype(F32) + states[m, i]
            ).astype(BF16)
            chain(m, i).start()

    def across(m, t, end):
        entering = jnp.concatenate([ent[m, i] for i in range(t, end)], axis=1)
        cols = slice(t * LANES, end * LANES)
        over = jnp.dot(conv[m, pairs + 1], entering, preferred_element_type=F32)
        gated = (base[m, :, cols] + decay_x[m, :, cols] * over) * gate[m, :, cols]
        squares_of = gated * gated
        total = squares_of[:, :LANES]
        for k in range(1, end - t):
            total = total + squares_of[:, k * LANES : (k + 1) * LANES]
        sq_acc[m] += total
        g[m, :, cols] = (gated * inner_gain[:, cols]).astype(BF16)

    def scan(m, between=(), ready=0):
        between = dict(between)
        done = 0
        for i in range(pairs):
            poll(m, i)
            if i in between:
                between[i]()
            if i == pairs - 1 or (i % 2 == 1 and i >= ready):
                while done <= i:
                    across(m, done, min(done + 2, i + 1))
                    done = min(done + 2, i + 1)

    def project_out(m):
        if m == 0:
            for copy in outs:
                copy.wait()
        if aligned:
            for d, j in lending:
                r = jnp.dot(g[m], w_out[d], preferred_element_type=F32)
                term[m, j] = r[:, :narrow].astype(BF16)
                lend(m, d, j).start()
                mine[m, d] = r[:, narrow:]
        else:
            for j in range(n_tensor):
                r = jnp.dot(
                    g[m], w_out[:, j * narrow : (j + 1) * narrow], preferred_element_type=F32
                )
                d = lax.rem(j // 2 - chip + chips, chips)
                term[m, j] = r.astype(BF16)
                mine[m, d] = jnp.where(core == j % 2, r, mine[m, d])
            for d, j in lending:
                lend(m, d, j).start()
        total = jnp.sum(sq_acc[m], axis=1, keepdims=True)
        sq_own[m] = jnp.broadcast_to(total, (rows, LANES)).T[:8]
        others(lambda j: squares(m, j).start())

    def combine(m):
        for d in range(1, chips):
            borrowed(m, d).wait_recv()
            for q in range(pieces):
                at = slice(q * some, (q + 1) * some)
                bundle[m, d - 1, at, :] = (
                    mine[m, d, at, :] + lent[m, chip_at(d), at, :].astype(F32)
                ).astype(BF16)
                part(m, d, q).start()

    def scale_rows(m):
        sq_all[m, me] = sq_own[m]
        others(lambda j: squared(m, j).wait_recv())
        total = sq_all[m, 0]
        for j in range(1, n_tensor):
            total = total + sq_all[m, j]
        scale = lax.rsqrt(total / (inner * n_tensor) + EPS)
        sq_acc[m] = jnp.broadcast_to(scale[0:1], (LANES, rows)).T
        borrowed(m, 0).wait_recv()

    def finish_piece(m, q):
        at = slice(q * some, (q + 1) * some)
        for d in range(1, chips):
            part(m, d, q).wait_recv()
        summed = mine[m, 0, at, :] + lent[m, chip, at, :].astype(F32)
        for d in range(1, chips):
            summed = summed + parts[m, d - 1, at, :].astype(F32)
        value = (u[m, me, at, :].astype(F32) + summed * sq_acc[m, at, 0:1]).astype(BF16)
        own[m, at, :] = value
        out[0, m, at, :] = value

        @pl.when(section < n_pipe - 1)
        def _():
            relay(m, q).start()

    def finish(m):
        scale_rows(m)
        for q in range(pieces):
            finish_piece(m, q)

    first = section == 0
    weave = jnp.logical_and(first, place > 0)

    def next_input(m):
        for q in range(pieces):
            send_own(m, q)

    @pl.when(first)
    def _():
        hand_over(0)
        for m in range(1, micros):
            stage(m).wait()
            next_input(m)

    @pl.when(section > 0)
    def _():
        forward(0)
        hand_over(0)

    take_input(0)
    project(0)
    pl.when(jnp.logical_not(weave))(lambda: convolve(0))
    project_gate(0)
    pl.when(weave)(lambda: convolve(0))
    count = tiles - pairs
    third = pairs // 3 // 2 * 2 + 2

    def spread_out(steps, start, stop):
        slots = {}
        for k, step in enumerate(steps):
            slots.setdefault(start + k * (stop - start) // len(steps), []).append(step)

        def run(held):
            for step in held:
                step()

        return {at: functools.partial(run, held) for at, held in slots.items()}

    for m in range(1, micros):
        ahead = m - 1
        halves = [
            lambda: inside_some(ahead, 0, middle),
            lambda: inside_some(ahead, middle, pairs),
        ]
        gates = [lambda: gate_some(m, 0, third), lambda: gate_some(m, third, pairs)]
        fresh = [
            lambda: inside_some(m, 0, middle),
            lambda: inside_some(m, middle, pairs),
        ]
        pieces_of = [lambda q=q: finish_piece(ahead, q) for q in range(pieces)]
        pieces_of[0] = lambda: (scale_rows(ahead), finish_piece(ahead, 0))

        @pl.when(weave)
        def _():
            work = halves + [
                lambda: (hand_over(m), take_input(m)),
                lambda: multiply(m, pairs, 0, count, w_state),
                lambda: multiply(m, 0, 0, third, w_inner),
                lambda: (multiply(m, 0, third, pairs, w_inner), send_rim(m)),
                lambda: step_sizes(m),
            ] + gates
            scan(ahead, spread_out(work, 0, pairs - 1), 2)
            project_out(ahead)
            combine(ahead)
            convolve(m)
            inside(m)
            pl.when(place == n_seq - 1)(lambda: finish(ahead))
            slots = spread_out(pieces_of, pairs // 5, pairs * 8 // 10)
            scan(
                m,
                {
                    at: (lambda step=step: pl.when(place < n_seq - 1)(step))
                    for at, step in slots.items()
                },
            )

        @pl.when(section > 0)
        def _():
            forward(m)
            work = halves
            slots = spread_out(halves, 0, 2)
            scan(ahead, slots, 2)
            hand_over(m)
            take_input(m)
            project(m)
            convolve(m)
            work = [lambda: project_out(ahead), lambda: combine(ahead)] + gates + fresh
            scan(m, spread_out(work, pairs // 5, pairs - 2), pairs - 3)

        @pl.when(jnp.logical_and(first, place == 0))
        def _():
            inside(ahead)
            hand_over(m)
            scan(ahead)
            project_out(ahead)
            combine(ahead)
            take_input(m)
            project(m)
            pieces_of[0]()
            convolve(m)
            pieces_of[1]()
            project_gate(m)
            for piece in pieces_of[2:]:
                piece()
            inside(m)
            scan(m)

    project_out(micros - 1)
    combine(micros - 1)

    @pl.when(section > 0)
    def _():
        for m in range(micros - 1):
            finish(m)

    finish(micros - 1)

    def drain(m, _):
        for q in range(pieces):
            near(m, q).wait_send()
            for d in range(1, chips):
                cross(m, d, q).wait_send()
                hand(m, d, q).wait_send()
        for d, j in lending:
            lend(m, d, j).wait_send()
        for q in range(pieces):
            for d in range(1, chips):
                part(m, d, q).wait_send()
        others(lambda j: squares(m, j).wait_send())

        @pl.when(place < n_seq - 1)
        def _():
            rim_copy(m).wait_send()

            def one(i, _):
                chain(m, i).wait_send()
                return 0

            lax.fori_loop(0, pairs, one, 0)

        @pl.when(section < n_pipe - 1)
        def _():
            for q in range(pieces):
                relay(m, q).wait_send()

        return 0

    lax.fori_loop(0, micros, drain, 0)


def shards(sizes, *args):
    tokens, prenorm, gate_w, inner_w, state_w, step_w = args[:6]
    n_pipe, n_tensor, n_seq = sizes
    micros, rows, narrow = tokens.shape
    width = prenorm.shape[1]
    inner = inner_w.shape[2]
    maps = state_w.shape[2]
    heads = step_w.shape[2]
    pairs = inner // LANES
    wide = inner + maps
    step_w = jnp.swapaxes(step_w, 1, 2)
    inner_taps, state_taps = (jnp.swapaxes(a, 0, 1) for a in args[6:8])
    args = (tokens, prenorm, gate_w, inner_w, state_w, step_w, inner_taps, state_taps) + args[8:]
    edge = 8
    chips = n_tensor // 2
    pieces = 4
    vmem = pl.BlockSpec(memory_space=pltpu.VMEM)
    far = pl.BlockSpec(memory_space=pltpu.HBM)
    dma = pltpu.SemaphoreType.DMA
    V = pltpu.VMEM
    return pl.pallas_call(
        functools.partial(kernel, sizes),
        out_shape=pltpu.VMEM((1, micros, rows, narrow), BF16),
        in_specs=[far] * len(args),
        out_specs=vmem,
        scratch_shapes=[
            V((1, width), F32),
            V(inner_taps.shape, F32),
            V(state_taps.shape, F32),
            V((1, heads), F32),
            V((1, heads), F32),
            V((1, heads), F32),
            V((1, inner), F32),
            V((width, inner), BF16),
            V((width, inner), BF16),
            V((width, maps), BF16),
            V((heads, width), BF16),
            V((chips, inner, 2 * narrow) if narrow % LANES == 0 else (inner, width), BF16),
            V((micros, n_tensor, rows, narrow), BF16),
            V((micros, rows, width), BF16),
            V((micros, wide // LANES, edge + rows, LANES), F32),
            V((micros, wide // LANES, rows, LANES), BF16),
            V((micros, rows, inner), F32),
            V((8, LANES), F32),
            V((width, LANES), BF16),
            V((rows, 3 * rows), BF16),
            V((2 * LANES, inner), BF16),
            V((2 * LANES, heads * rows), BF16),
            V((1, inner), F32),
            V((micros, rows, 2 * LANES), BF16),
            V((micros, LANES, rows), F32),
            V((micros, rows, inner), F32),
            V((micros, rows, inner), F32),
            V((micros, LANES, rows), BF16),
            V((micros, rows, rows), F32),
            V((micros, pairs, LANES, LANES), F32),
            V((micros, pairs, LANES, LANES), BF16),
            V((micros, pairs, LANES, LANES), BF16),
            V((micros, rows, inner), F32),
            V((micros, rows, inner), BF16),
            V((micros, rows, LANES), F32),
            V((micros, 8, rows), F32),
            V((micros, n_tensor, 8, rows), F32),
            V((micros, n_tensor, rows, narrow), BF16),
            V((micros, chips, rows, narrow), F32),
            V((micros, chips, rows, narrow), BF16),
            V((micros, chips - 1, rows, narrow), BF16),
            V((micros, chips - 1, rows, narrow), BF16),
            V((micros, rows, narrow), BF16),
            dma((4 + n_tensor,)),
            dma((7,)),
            dma((micros,)),
            dma((micros, n_tensor, pieces)),
            dma((micros, n_tensor, pieces)),
            dma((micros,)),
            dma((micros,)),
            dma((micros, pairs)),
            dma((micros, pairs)),
            dma((micros, chips)),
            dma((micros, chips)),
            dma((micros, chips - 1, pieces)),
            dma((micros, chips - 1, pieces)),
            dma((micros, n_tensor)),
            dma((micros, n_tensor)),
            dma((micros, pieces)),
            dma((micros, pieces)),
        ],
        compiler_params=pltpu.CompilerParams(
            collective_id=0, has_side_effects=True, vmem_limit_bytes=60000 * 1024
        ),
    )(*args)


def solution(mesh):
    sizes = (mesh.shape["pipe"], mesh.shape["tensor"], mesh.shape["seq"])
    placed = (
        P(None, "seq", "tensor"),
        P("pipe", None),
        P("pipe", None, "tensor"),
        P("pipe", None, "tensor"),
        P("pipe", None, None),
        P("pipe", None, "tensor"),
        P("pipe", None, "tensor"),
        P("pipe", None, None),
        P("pipe", "tensor"),
        P("pipe", "tensor"),
        P("pipe", "tensor"),
        P("pipe", "tensor"),
        P("pipe", "tensor", None),
    )
    return jax.shard_map(
        functools.partial(shards, sizes),
        mesh=mesh,
        in_specs=placed,
        out_specs=P("pipe", None, "seq", "tensor"),
        check_vma=False,
    )
```

```python
import functools

import jax
import jax.numpy as jnp
from jax import lax
from jax.experimental import pallas as pl
from jax.experimental.pallas import tpu as pltpu
from jax.sharding import PartitionSpec as P

EPS = 1e-05
LANES = 128
MESH = pl.DeviceIdType.MESH
F32 = jnp.float32
BF16 = jnp.bfloat16


LOG2E = 1.4426950408889634
CAP = 126.0


def half_silu(h):
    return h + h * jnp.tanh(h)


def split(v, parts):
    pieces = []
    for _ in range(parts - 1):
        piece = v.astype(BF16)
        pieces.append(piece)
        v = v - piece.astype(F32)
    return pieces + [v.astype(BF16)]


def remote(src, dst, send, recv, where):
    return pltpu.make_async_remote_copy(
        src_ref=src, dst_ref=dst, send_sem=send, recv_sem=recv, device_id=where, device_id_type=MESH
    )


def kernel(
    sizes,
    tokens,
    prenorm_hbm,
    gate_hbm,
    inner_hbm,
    state_hbm,
    step_hbm,
    inner_taps_hbm,
    state_taps_hbm,
    step_bias_hbm,
    decay_rate_hbm,
    skip_scale_hbm,
    inner_gain_hbm,
    out_hbm,
    out,
    prenorm,
    inner_taps,
    state_taps,
    step_bias,
    decay_rate,
    skip_scale,
    inner_gain,
    w_gate,
    w_inner,
    w_state,
    w_step,
    w_out,
    u,
    ni,
    raw,
    conv,
    gate,
    rates,
    w_step_t,
    later3,
    spread_w,
    spread_c,
    skips,
    lhs_c,
    fall_t,
    weight_x,
    decay_x,
    b_t,
    scores,
    states,
    ent,
    snd,
    base,
    g,
    sq_acc,
    sq_own,
    sq_all,
    term,
    mine,
    lent,
    bundle,
    parts,
    own,
    w_sem,
    v_sem,
    t_sem,
    ag_send,
    ag_recv,
    near_recv,
    rim_send,
    rim_recv,
    ch_send,
    ch_recv,
    lend_send,
    lend_recv,
    rs_send,
    rs_recv,
    sq_send,
    sq_recv,
    pipe_send,
    pipe_recv,
):
    n_pipe, n_tensor, n_seq = sizes
    micros, rows, narrow = own.shape
    width = prenorm.shape[1]
    inner = w_inner.shape[1]
    heads = step_bias.shape[1]
    head_size = inner // heads
    pack = LANES // head_size
    pairs = inner // LANES
    tiles = raw.shape[1]
    reach = inner_taps.shape[0] - 2
    edge = raw.shape[2] - rows
    section = lax.axis_index("pipe")
    me = lax.axis_index("tensor")
    place = lax.axis_index("seq")
    half = LANES // 2
    wide = 2 * LANES

    core = lax.rem(me, 2)
    chip = me // 2
    partner = me + 1 - 2 * core
    chips = n_tensor // 2
    pieces = near_recv.shape[1]
    some = rows // pieces
    aligned = w_out.ndim == 3

    def chip_at(d):
        return lax.rem(chip + d, chips)

    order = list(range(1, chips)) + [0]
    lending = [(d, 2 * chip_at(d) + 1 - core) for d in order]
    keeping = [(d, 2 * chip_at(d) + core) for d in order]

    def load(src, dst, k):
        return pltpu.make_async_copy(src, dst, w_sem.at[k])

    loads = [
        load(step_hbm.at[0], w_step, 0),
        load(state_hbm.at[0], w_state, 1),
        load(inner_hbm.at[0], w_inner, 2),
        load(gate_hbm.at[0], w_gate, 3),
    ]
    if aligned:
        outs = [
            load(
                out_hbm.at[0, :, pl.ds(pl.multiple_of(j * narrow, LANES), narrow)],
                w_out.at[d, :, pl.ds(side * narrow, narrow)],
                4 + 2 * d + side,
            )
            for pair in zip(lending, keeping)
            for side, (d, j) in enumerate(pair)
        ]
    else:
        outs = [load(out_hbm.at[0], w_out, 4)]
    vectors = [
        pltpu.make_async_copy(src, dst, v_sem.at[k])
        for k, (src, dst) in enumerate(
            (
                (prenorm_hbm, prenorm),
                (inner_taps_hbm, inner_taps),
                (state_taps_hbm, state_taps),
                (step_bias_hbm, step_bias),
                (decay_rate_hbm, decay_rate),
                (skip_scale_hbm, skip_scale),
                (inner_gain_hbm, inner_gain),
            )
        )
    ]

    def stage(m):
        return pltpu.make_async_copy(tokens.at[m], u.at[m, me], t_sem.at[m])

    def at_chip(d):
        return 2 * chip_at(d) + core

    def gather(m, q, src, recv, where):
        block = u.at[m, src, pl.ds(q * some, some)]
        return remote(block, block, ag_send.at[m], recv, {"tensor": where})

    def near(m, q):
        return gather(m, q, me, near_recv.at[m, q], partner)

    def cross(m, d, q):
        return gather(m, q, me, ag_recv.at[m, d - 1, q], at_chip(d))

    def crossed(m, d, q):
        return gather(m, q, at_chip(chips - d), ag_recv.at[m, d - 1, q], partner)

    def hand(m, d, q):
        return gather(m, q, at_chip(chips - d), near_recv.at[m, q], partner)

    def gathered(m, q):
        half_of = u.at[m, pl.ds(0, chips), pl.ds(q * some, some)]
        return remote(half_of, half_of, ag_send.at[m], near_recv.at[m, q], {"tensor": partner})

    def bulk(block, send):
        return remote(block, block, send, near_recv.at[0, 0], {"tensor": partner})

    def send_own(m, q):
        for d in range(1, chips):
            cross(m, d, q).start()
        near(m, q).start()

    groups = [(0, tiles)]

    def rim_copy(m, k):
        at = pl.ds(groups[k][0], groups[k][1] - groups[k][0])
        return remote(
            raw.at[m, at, pl.ds(rows, edge)],
            raw.at[m, at, pl.ds(0, edge)],
            rim_send.at[m, k],
            rim_recv.at[m, k],
            {"seq": lax.rem(place + 1, n_seq)},
        )

    def chain(m, i):
        return remote(
            snd.at[m, i],
            ent.at[m, i],
            ch_send.at[m],
            ch_recv.at[m, i],
            {"seq": lax.rem(place + 1, n_seq)},
        )

    def lend(m, d, j):
        to = chip_at(d)
        return remote(
            term.at[m, j], lent.at[m, to], lend_send.at[m], lend_recv.at[m, to], {"tensor": partner}
        )

    def borrowed(m, d):
        to = chip_at(d)
        return remote(
            lent.at[m, to], lent.at[m, to], lend_send.at[m], lend_recv.at[m, to], {"tensor": partner}
        )

    def part(m, d, q):
        at = pl.ds(q * some, some)
        return remote(
            bundle.at[m, d - 1, at],
            parts.at[m, d - 1, at],
            rs_send.at[m],
            rs_recv.at[m, d - 1, q],
            {"tensor": at_chip(d)},
        )

    def squares(m, j):
        return remote(
            sq_own.at[m], sq_all.at[m, me], sq_send.at[m], sq_recv.at[m], {"tensor": j}
        )

    def squared(m):
        block = sq_all.at[m, pl.ds(0, n_tensor - 1)]
        return remote(block, block, sq_send.at[m], sq_recv.at[m], {"tensor": partner})

    def relay(m, q):
        return remote(
            own.at[m, pl.ds(q * some, some)],
            u.at[m, me, pl.ds(q * some, some)],
            pipe_send.at[m],
            pipe_recv.at[m, q],
            {"pipe": lax.rem(section + 1, n_pipe)},
        )

    def others(action):
        for j in range(n_tensor):
            pl.when(me != j)(functools.partial(action, j))

    @pl.when(section == 0)
    def _():
        stage(0).start()

    for copy in vectors + loads[:1]:
        copy.start()

    @pl.when(section == 0)
    def _():
        for m in range(1, micros):
            stage(m).start()

    barrier = pltpu.get_barrier_semaphore()

    def greet(where):
        pl.semaphore_signal(barrier, inc=1, device_id=where, device_id_type=MESH)

    others(lambda j: greet({"tensor": j}))
    partners = n_tensor - 1
    for axis, index, count in (("seq", place, n_seq), ("pipe", section, n_pipe)):
        pl.when(index > 0)(functools.partial(greet, {axis: index - 1}))
        pl.when(index < count - 1)(functools.partial(greet, {axis: index + 1}))
        partners = partners + jnp.where(index > 0, 1, 0) + jnp.where(index < count - 1, 1, 0)
    pl.semaphore_wait(barrier, partners)

    @pl.when(section == 0)
    def _():
        stage(0).wait()
        for q in range(pieces):
            send_own(0, q)

    for copy in loads[1:]:
        copy.start()

    for copy in outs:
        copy.start()
    for copy in vectors:
        copy.wait()
    inner_taps[...] = inner_taps[...] * 0.5
    state_taps[...] = state_taps[...] * 0.5
    rates[...] = jnp.zeros_like(rates)
    rates[0:1, :heads] = decay_rate[...] * (-LOG2E)
    rates[1:2, :heads] = step_bias[...]
    rates[2:3, :heads] = skip_scale[...]
    sq_acc[...] = jnp.zeros_like(sq_acc)

    @pl.when(place == 0)
    def _():
        for m in range(micros):
            raw[m, :, 0:edge, :] = jnp.zeros((tiles, edge, LANES), F32)
        ent[...] = jnp.zeros_like(ent)

    low = lax.broadcasted_iota(jnp.int32, (rows, LANES), 0)
    lane = lax.broadcasted_iota(jnp.int32, (rows, LANES), 1)
    later = low >= lane
    for k in range(3):
        later3[:, k * rows : (k + 1) * rows] = later.astype(F32).astype(BF16)

    def spreading(columns, size, first):
        k = lax.broadcasted_iota(jnp.int32, (wide, columns), 0)
        at = lax.broadcasted_iota(jnp.int32, (wide, columns), 1) + first
        row = k
        for start in (half, LANES, LANES + half):
            if size == head_size and start != LANES:
                continue
            row = jnp.where(k >= start, k - start, row)
        if size != head_size:
            row = jnp.where(jnp.logical_and(k >= half, k < LANES), LANES, row)
        inside = jnp.logical_and(at >= row * size, at < (row + 1) * size)
        return jnp.where(inside, 1.0, 0.0).astype(BF16)

    def fill_w(t, _):
        at = pl.multiple_of(t * LANES, LANES)
        spread_w[:, pl.ds(at, LANES)] = spreading(LANES, head_size, at)
        return 0

    def fill_c(t, _):
        at = pl.multiple_of(t * LANES, LANES)
        spread_c[:, pl.ds(at, LANES)] = spreading(LANES, rows, at)
        return 0

    lax.fori_loop(0, pairs, fill_w, 0)
    lax.fori_loop(0, heads, fill_c, 0)
    for t in range(pairs):
        cols = slice(t * LANES, (t + 1) * LANES)
        r = lax.broadcasted_iota(jnp.int32, (8, LANES), 0)
        whole = jnp.broadcast_to(rates[2:3], (8, LANES))
        h0 = lax.broadcasted_iota(jnp.int32, (8, LANES), 1)
        row = jnp.zeros((8, LANES), F32)
        for k in range(pack):
            one = jnp.sum(jnp.where(h0 == t * pack + k, whole, 0.0), axis=1, keepdims=True)
            row = jnp.where(h0 >= k * head_size, one, row)
        skips[:, cols] = row[0:1]

    loads[0].wait()
    w_step_t[...] = (
        jnp.concatenate([w_step[...].astype(F32), jnp.zeros((LANES - heads, width), F32)], axis=0)
        .T.astype(BF16)
    )

    def forward_piece(m, q):
        relay(m, q).wait_recv()
        send_own(m, q)

    def forward(m):
        for q in range(pieces):
            forward_piece(m, q)

    def hand_piece(m, q):
        for d in range(1, chips):
            crossed(m, d, q).wait_recv()
            hand(m, d, q).start()

    def hand_over(m):
        for q in range(pieces):
            hand_piece(m, q)

    def take_input(m):
        for q in range(pieces):
            gathered(m, q).wait_recv()
            at = slice(q * some, (q + 1) * some)
            total = jnp.zeros((some, 1), F32)
            for j in range(n_tensor):
                v = u[m, j, at, :].astype(F32)
                total = total + jnp.sum(v * v, axis=1, keepdims=True)
            scale = lax.rsqrt(total / width + EPS)
            for j in range(n_tensor):
                cols = slice(j * narrow, (j + 1) * narrow)
                v = u[m, j, at, :].astype(F32)
                ni[m, at, cols] = (v * scale * prenorm[:, cols]).astype(BF16)

    def multiply(m, first, begin, end, weights):
        for t in range(begin, end, 2):
            stop = min(t + 2, end)
            r = jnp.dot(ni[m], weights[:, t * LANES : stop * LANES], preferred_element_type=F32)
            for k in range(t, stop):
                raw[m, first + k, edge:, :] = r[:, (k - t) * LANES : (k - t + 1) * LANES]

    def send_rim(m, keys):
        @pl.when(place < n_seq - 1)
        def _():
            for k in keys:
                rim_copy(m, k).start()

    def take_rim(m, keys):
        @pl.when(place > 0)
        def _():
            for k in keys:
                rim_copy(m, k).wait_recv()

    def step_sizes(m):
        v = jnp.dot(ni[m], w_step_t[...], preferred_element_type=F32) + rates[1:2]
        step = jnp.maximum(v, 0.0) + jnp.log1p(jnp.exp(-jnp.abs(v)))
        cum = jnp.dot(
            later3[...],
            jnp.concatenate(split(step * rates[0:1], 3), axis=0),
            preferred_element_type=F32,
        )
        fall_t[m] = (cum - jnp.log(step) * LOG2E).T
        weight = jnp.exp2(cum[rows - 1 :] - cum) * step
        both = jnp.concatenate(
            [
                jnp.concatenate(split(weight, 2), axis=1),
                jnp.concatenate(split(jnp.exp2(cum), 2), axis=1),
            ],
            axis=0,
        )
        for t in range(0, pairs, 2):
            cols = slice(t * LANES, min(t + 2, pairs) * LANES)
            r = jnp.dot(both, spread_w[:, cols], preferred_element_type=F32)
            weight_x[m, :, cols] = r[:rows]
            decay_x[m, :, cols] = r[rows:]
        high, mid, last = split(cum, 3)
        last = pltpu.roll(last.astype(F32), half, 1)
        lhs_c[m] = jnp.concatenate([high, (mid.astype(F32) + last).astype(BF16)], axis=1)

    every = range(len(groups))
    early = pairs * 2 // 5 // 2 * 2

    def project(m):
        step_sizes(m)
        multiply(m, pairs, 0, tiles - pairs, w_state)
        multiply(m, 0, 0, pairs, w_inner)
        send_rim(m, every)

    def gate_some(m, begin, end):
        for t in range(begin, end, 2):
            cols = slice(t * LANES, min(t + 2, end) * LANES)
            r = jnp.dot(ni[m], w_gate[:, cols], preferred_element_type=F32)
            gate[m, :, cols] = half_silu(0.5 * r)

    def project_gate(m):
        gate_some(m, 0, pairs)

    def tile(m, t):
        taps, at = (inner_taps, t) if t < pairs else (state_taps, t - pairs)
        cols = slice(at * LANES, (at + 1) * LANES)
        total = jnp.broadcast_to(taps[reach + 1, :, cols], (rows, LANES))
        for k in range(reach + 1):
            total = total + taps[k, :, cols] * raw[m, t, pl.ds(edge - reach + k, rows), :]
        result = half_silu(total).astype(BF16)
        conv[m, t] = result
        return result

    def convolve_maps(m):
        b = tile(m, pairs)
        c = tile(m, pairs + 1)
        b_t[m] = b.astype(F32).T.astype(BF16)
        found = lax.dot_general(c, b, (((1,), (1,)), ((), ())), preferred_element_type=F32)
        scores[m] = jnp.where(later, found, 0.0)

    def convolve_some(m, begin, end):
        for t in range(begin, end, 2):
            stop = min(t + 2, end)
            weighted = jnp.concatenate(
                [
                    (
                        tile(m, k).astype(F32) * weight_x[m, :, k * LANES : (k + 1) * LANES]
                    ).astype(BF16)
                    for k in range(t, stop)
                ],
                axis=1,
            )
            r = jnp.dot(b_t[m], weighted, preferred_element_type=F32)
            for k in range(t, stop):
                one = r[:, (k - t) * LANES : (k - t + 1) * LANES]
                states[m, k] = one
                snd[m, k] = one.astype(BF16)

        @pl.when(place == 0)
        def _():
            for i in range(begin, end):
                chain(m, i).start()

    middle = pairs // 4 * 2

    def convolve(m):
        take_rim(m, every)
        convolve_maps(m)
        convolve_some(m, 0, middle)
        convolve_some(m, middle, pairs)

    def inside_some(m, begin, end):
        for i in range(begin, end):
            spread = jnp.dot(
                lhs_c[m],
                spread_c[:, i * pack * rows : (i + 1) * pack * rows],
                preferred_element_type=F32,
            )
            mixing = []
            for k in range(pack):
                fall = spread[:, k * rows : (k + 1) * rows] - fall_t[m, pl.ds(i * pack + k, 1), :]
                mixing.append((scores[m] * jnp.exp2(jnp.minimum(fall, CAP))).astype(BF16))
            x = conv[m, i]
            apart = [
                jnp.where(jnp.logical_and(lane >= k * head_size, lane < (k + 1) * head_size), x, 0.0)
                for k in range(pack)
            ]
            result = jnp.dot(
                jnp.concatenate(mixing, axis=1),
                jnp.concatenate([a.astype(BF16) for a in apart], axis=0),
                preferred_element_type=F32,
            )
            cols = slice(i * LANES, (i + 1) * LANES)
            base[m, :, cols] = result + skips[:, cols] * x.astype(F32)

    def inside(m):
        inside_some(m, 0, pairs)

    def poll(m, i):
        @pl.when(place > 0)
        def _():
            chain(m, i).wait_recv()

        @pl.when(jnp.logical_and(place > 0, place < n_seq - 1))
        def _():
            cols = slice(i * LANES, (i + 1) * LANES)
            snd[m, i] = (
                decay_x[m, rows - 1 :, cols] * ent[m, i].astype(F32) + states[m, i]
            ).astype(BF16)
            chain(m, i).start()

    def across(m, t, end):
        entering = jnp.concatenate([ent[m, i] for i in range(t, end)], axis=1)
        cols = slice(t * LANES, end * LANES)
        over = jnp.dot(conv[m, pairs + 1], entering, preferred_element_type=F32)
        gated = (base[m, :, cols] + decay_x[m, :, cols] * over) * gate[m, :, cols]
        squares_of = gated * gated
        total = squares_of[:, :LANES]
        for k in range(1, end - t):
            total = total + squares_of[:, k * LANES : (k + 1) * LANES]
        sq_acc[m] += total
        g[m, :, cols] = (gated * inner_gain[:, cols]).astype(BF16)

    def scan(m, between=(), ready=0, start=0):
        between = dict(between)
        done = 0
        for i in range(start, pairs):
            poll(m, i)
            if i in between:
                between[i]()
            if i >= ready or i == pairs - 1:
                while done + 2 <= i + 1 or (i == pairs - 1 and done <= i):
                    across(m, done, min(done + 2, pairs))
                    done = min(done + 2, pairs)

    def project_out(m):
        if m == 0:
            for copy in outs:
                copy.wait()
        if aligned:
            for d, j in lending:
                if d > 0:
                    r = jnp.dot(g[m], w_out[d, :, :narrow], preferred_element_type=F32)
                    term[m, j] = r.astype(BF16)
                    lend(m, d, j).start()
                    mine[m, d] = jnp.dot(g[m], w_out[d, :, narrow:], preferred_element_type=F32)
                    continue
                r = jnp.dot(g[m], w_out[d], preferred_element_type=F32)
                term[m, j] = r[:, :narrow].astype(BF16)
                lend(m, d, j).start()
                mine[m, d] = r[:, narrow:]
        else:
            for j in range(n_tensor):
                r = jnp.dot(
                    g[m], w_out[:, j * narrow : (j + 1) * narrow], preferred_element_type=F32
                )
                d = lax.rem(j // 2 - chip + chips, chips)
                term[m, j] = r.astype(BF16)
                mine[m, d] = jnp.where(core == j % 2, r, mine[m, d])
            for d, j in lending:
                lend(m, d, j).start()
        total = jnp.sum(sq_acc[m], axis=1, keepdims=True)
        sq_own[m] = jnp.broadcast_to(total, (rows, LANES)).T[:8]
        others(lambda j: squares(m, j).start())

    def combine(m):
        for d in range(1, chips):
            borrowed(m, d).wait_recv()
            for q in range(pieces):
                at = slice(q * some, (q + 1) * some)
                bundle[m, d - 1, at, :] = (
                    mine[m, d, at, :] + lent[m, chip_at(d), at, :].astype(F32)
                ).astype(BF16)
                part(m, d, q).start()

    def scale_rows(m):
        squared(m).wait_recv()
        sq_all[m, me] = sq_own[m]
        total = sq_all[m, 0]
        for j in range(1, n_tensor):
            total = total + sq_all[m, j]
        scale = lax.rsqrt(total / (inner * n_tensor) + EPS)
        sq_acc[m] = jnp.broadcast_to(scale[0:1], (LANES, rows)).T
        borrowed(m, 0).wait_recv()

    def finish_piece(m, q):
        at = slice(q * some, (q + 1) * some)
        for d in range(1, chips):
            part(m, d, q).wait_recv()
        summed = mine[m, 0, at, :] + lent[m, chip, at, :].astype(F32)
        for d in range(1, chips):
            summed = summed + parts[m, d - 1, at, :].astype(F32)
        value = (u[m, me, at, :].astype(F32) + summed * sq_acc[m, at, 0:1]).astype(BF16)
        own[m, at, :] = value
        out[0, m, at, :] = value

        @pl.when(section < n_pipe - 1)
        def _():
            relay(m, q).start()

    def finish(m):
        scale_rows(m)
        for q in range(pieces):
            finish_piece(m, q)

    first = section == 0
    weave = jnp.logical_and(first, place > 0)

    def next_input(m):
        for q in range(pieces):
            send_own(m, q)

    @pl.when(first)
    def _():
        hand_over(0)
        for m in range(1, micros):
            stage(m).wait()
            next_input(m)

    @pl.when(section > 0)
    def _():
        forward(0)
        hand_over(0)

    take_input(0)
    for copy in loads[1:]:
        copy.wait()
    count = tiles - pairs
    third = pairs // 3 // 2 * 2 + 2
    project(0)
    pl.when(jnp.logical_not(weave))(lambda: convolve(0))

    @pl.when(weave)
    def _():
        project_gate(0)
        convolve(0)

    def spread_out(steps, start, stop):
        slots = {}
        for k, step in enumerate(steps):
            slots.setdefault(start + k * (stop - start) // len(steps), []).append(step)

        def run(held):
            for step in held:
                step()

        return {at: functools.partial(run, held) for at, held in slots.items()}

    for m in range(1, micros):
        ahead = m - 1

        def gates(m):
            return [lambda: gate_some(m, 0, third), lambda: gate_some(m, third, pairs)]

        def insides(m):
            return [lambda: inside_some(m, 0, middle), lambda: inside_some(m, middle, pairs)]

        pieces_of = [lambda q=q: finish_piece(ahead, q) for q in range(pieces)]

        def first_piece():
            scale_rows(ahead)
            finish_piece(ahead, 0)

        pieces_of[0] = first_piece

        @pl.when(weave)
        def _():
            hand_over(m)
            work = insides(ahead) + [
                lambda: take_input(m),
                lambda: step_sizes(m),
                lambda: multiply(m, pairs, 0, count, w_state),
                lambda: multiply(m, 0, 0, third, w_inner),
                lambda: (multiply(m, 0, third, pairs, w_inner), send_rim(m, every)),
            ] + gates(m)
            scan(ahead, spread_out(work, 0, pairs - 1), 2)
            project_out(ahead)
            convolve(m)
            combine(ahead)
            slots = {0: [insides(m)[0]], 1: [insides(m)[1]]}
            slots[1].append(lambda: pl.when(place == n_seq - 1)(lambda: finish(ahead)))
            for at, step in zip((3, 5, 7), pieces_of):
                at = min(at, pairs - 1)
                slots.setdefault(at, []).append(
                    lambda step=step: pl.when(place < n_seq - 1)(step)
                )
            scan(
                m,
                {
                    at: (lambda held=held: [step() for step in held])
                    for at, held in slots.items()
                },
                2,
            )
            for step in pieces_of[3:]:
                pl.when(place < n_seq - 1)(step)

        @pl.when(section > 0)
        def _():
            share = pieces // 2

            def forward_some(begin, end):
                for q in range(begin, end):
                    forward_piece(m, q)

            def with_gate(k):
                gates(ahead)[k]()
                forward_some(share + k * share // 2, share + (k + 1) * share // 2)

            events = [
                (0, lambda: forward_some(0, share)),
                (1, lambda: with_gate(0)),
                (2, lambda: with_gate(1)),
                (3, insides(ahead)[0]),
                (5, insides(ahead)[1]),
            ]
            for q in range(pieces):
                events.append((4 + q * 4 // pieces, functools.partial(hand_piece, m, q)))
            events += [(9, lambda: take_input(m)), (9, lambda: project(m))]
            events.sort(key=lambda event: event[0])
            for i in range(pairs):
                poll(ahead, i)
                for at, step in events:
                    if at * pairs // 10 == i:
                        step()
            convolve(m)
            for i in range(early):
                poll(m, i)

            def cross_over():
                for t in range(0, pairs, 2):
                    across(ahead, t, min(t + 2, pairs))

            work = [
                cross_over,
                lambda: project_out(ahead),
                lambda: combine(ahead),
            ] + gates(m) + insides(m)
            scan(m, spread_out(work, early, pairs - 2), pairs - 2, early)

        @pl.when(jnp.logical_and(first, place == 0))
        def _():
            if ahead == 0:
                project_gate(ahead)
            inside(ahead)
            hand_over(m)
            scan(ahead)
            project_out(ahead)
            take_input(m)
            combine(ahead)
            project(m)
            convolve(m)
            for piece in pieces_of[: pieces // 2]:
                piece()
            project_gate(m)
            for piece in pieces_of[pieces // 2 :]:
                piece()
            inside(m)
            scan(m)

    project_out(micros - 1)
    combine(micros - 1)

    def settle(m):
        bulk(u.at[m, pl.ds(0, n_tensor - 1)], ag_send.at[m]).wait_send()
        bulk(lent.at[m], lend_send.at[m]).wait_send()

        @pl.when(place < n_seq - 1)
        def _():
            for k in every:
                rim_copy(m, k).wait_send()
            bulk(snd.at[m], ch_send.at[m]).wait_send()

    def settle_sums(m):
        squared(m).wait_send()
        bulk(bundle.at[m], rs_send.at[m]).wait_send()

        @pl.when(section < n_pipe - 1)
        def _():
            bulk(own.at[m], pipe_send.at[m]).wait_send()

    @pl.when(section > 0)
    def _():
        for m in range(micros - 1):
            finish(m)

    for m in range(micros):
        settle(m)
    for m in range(micros - 1):
        settle_sums(m)
    finish(micros - 1)
    settle_sums(micros - 1)


def shards(sizes, *args):
    tokens, prenorm, gate_w, inner_w, state_w, step_w = args[:6]
    n_pipe, n_tensor, n_seq = sizes
    micros, rows, narrow = tokens.shape
    width = prenorm.shape[1]
    inner = inner_w.shape[2]
    maps = state_w.shape[2]
    heads = step_w.shape[2]
    pairs = inner // LANES
    wide = inner + maps
    step_w = jnp.swapaxes(step_w, 1, 2)
    inner_taps, state_taps = (jnp.swapaxes(a, 0, 1) for a in args[6:8])
    args = (tokens, prenorm, gate_w, inner_w, state_w, step_w, inner_taps, state_taps) + args[8:]
    edge = 8
    chips = n_tensor // 2
    pieces = 4
    vmem = pl.BlockSpec(memory_space=pltpu.VMEM)
    far = pl.BlockSpec(memory_space=pltpu.HBM)
    dma = pltpu.SemaphoreType.DMA
    V = pltpu.VMEM
    return pl.pallas_call(
        functools.partial(kernel, sizes),
        out_shape=pltpu.VMEM((1, micros, rows, narrow), BF16),
        in_specs=[far] * len(args),
        out_specs=vmem,
        scratch_shapes=[
            V((1, width), F32),
            V(inner_taps.shape, F32),
            V(state_taps.shape, F32),
            V((1, heads), F32),
            V((1, heads), F32),
            V((1, heads), F32),
            V((1, inner), F32),
            V((width, inner), BF16),
            V((width, inner), BF16),
            V((width, maps), BF16),
            V((heads, width), BF16),
            V((chips, inner, 2 * narrow) if narrow % LANES == 0 else (inner, width), BF16),
            V((micros, n_tensor, rows, narrow), BF16),
            V((micros, rows, width), BF16),
            V((micros, wide // LANES, edge + rows, LANES), F32),
            V((micros, wide // LANES, rows, LANES), BF16),
            V((micros, rows, inner), F32),
            V((8, LANES), F32),
            V((width, LANES), BF16),
            V((rows, 3 * rows), BF16),
            V((2 * LANES, inner), BF16),
            V((2 * LANES, heads * rows), BF16),
            V((1, inner), F32),
            V((micros, rows, 2 * LANES), BF16),
            V((micros, LANES, rows), F32),
            V((micros, rows, inner), F32),
            V((micros, rows, inner), F32),
            V((micros, LANES, rows), BF16),
            V((micros, rows, rows), F32),
            V((micros, pairs, LANES, LANES), F32),
            V((micros, pairs, LANES, LANES), BF16),
            V((micros, pairs, LANES, LANES), BF16),
            V((micros, rows, inner), F32),
            V((micros, rows, inner), BF16),
            V((micros, rows, LANES), F32),
            V((micros, 8, rows), F32),
            V((micros, n_tensor, 8, rows), F32),
            V((micros, n_tensor, rows, narrow), BF16),
            V((micros, chips, rows, narrow), F32),
            V((micros, chips, rows, narrow), BF16),
            V((micros, chips - 1, rows, narrow), BF16),
            V((micros, chips - 1, rows, narrow), BF16),
            V((micros, rows, narrow), BF16),
            dma((4 + n_tensor,)),
            dma((7,)),
            dma((micros,)),
            dma((micros,)),
            dma((micros, chips - 1, pieces)),
            dma((micros, pieces)),
            dma((micros, 1)),
            dma((micros, 1)),
            dma((micros,)),
            dma((micros, pairs)),
            dma((micros,)),
            dma((micros, chips)),
            dma((micros,)),
            dma((micros, chips - 1, pieces)),
            dma((micros,)),
            dma((micros,)),
            dma((micros,)),
            dma((micros, pieces)),
        ],
        compiler_params=pltpu.CompilerParams(
            collective_id=0, has_side_effects=True, vmem_limit_bytes=60000 * 1024
        ),
    )(*args)


def solution(mesh):
    sizes = (mesh.shape["pipe"], mesh.shape["tensor"], mesh.shape["seq"])
    placed = (
        P(None, "seq", "tensor"),
        P("pipe", None),
        P("pipe", None, "tensor"),
        P("pipe", None, "tensor"),
        P("pipe", None, None),
        P("pipe", None, "tensor"),
        P("pipe", None, "tensor"),
        P("pipe", None, None),
        P("pipe", "tensor"),
        P("pipe", "tensor"),
        P("pipe", "tensor"),
        P("pipe", "tensor"),
        P("pipe", "tensor", None),
    )
    return jax.shard_map(
        functools.partial(shards, sizes),
        mesh=mesh,
        in_specs=placed,
        out_specs=P("pipe", None, "seq", "tensor"),
        check_vma=False,
    )
```

```python
import functools

import jax
import jax.numpy as jnp
from jax import lax
from jax.experimental import pallas as pl
from jax.experimental.pallas import tpu as pltpu
from jax.sharding import PartitionSpec as P

EPS = 1e-05
LANES = 128
MESH = pl.DeviceIdType.MESH
F32 = jnp.float32
BF16 = jnp.bfloat16


LOG2E = 1.4426950408889634
CAP = 126.0


def half_silu(h):
    return h + h * jnp.tanh(h)


def split(v, parts):
    pieces = []
    for _ in range(parts - 1):
        piece = v.astype(BF16)
        pieces.append(piece)
        v = v - piece.astype(F32)
    return pieces + [v.astype(BF16)]


def remote(src, dst, send, recv, where):
    return pltpu.make_async_remote_copy(
        src_ref=src, dst_ref=dst, send_sem=send, recv_sem=recv, device_id=where, device_id_type=MESH
    )


def kernel(
    sizes,
    tokens,
    prenorm_hbm,
    gate_hbm,
    inner_hbm,
    state_hbm,
    step_hbm,
    inner_taps_hbm,
    state_taps_hbm,
    step_bias_hbm,
    decay_rate_hbm,
    skip_scale_hbm,
    inner_gain_hbm,
    out_hbm,
    out,
    prenorm,
    inner_taps,
    state_taps,
    step_bias,
    decay_rate,
    skip_scale,
    inner_gain,
    w_gate,
    w_inner,
    w_state,
    w_step,
    w_out,
    u,
    ni,
    raw,
    conv,
    gate,
    rates,
    w_step_t,
    later3,
    spread_w,
    spread_c,
    skips,
    lhs_c,
    fall_t,
    weight_x,
    decay_x,
    b_t,
    scores,
    states,
    ent,
    snd,
    base,
    g,
    sq_acc,
    sq_own,
    sq_all,
    term,
    mine,
    lent,
    bundle,
    parts,
    own,
    w_sem,
    v_sem,
    t_sem,
    ag_send,
    ag_recv,
    near_recv,
    rim_send,
    rim_recv,
    ch_send,
    ch_recv,
    lend_send,
    lend_recv,
    rs_send,
    rs_recv,
    sq_send,
    sq_recv,
    pipe_send,
    pipe_recv,
):
    n_pipe, n_tensor, n_seq = sizes
    micros, rows, narrow = own.shape
    width = prenorm.shape[1]
    inner = w_inner.shape[1]
    heads = step_bias.shape[1]
    head_size = inner // heads
    pack = LANES // head_size
    pairs = inner // LANES
    tiles = raw.shape[1]
    reach = inner_taps.shape[0] - 2
    edge = raw.shape[2] - rows
    section = lax.axis_index("pipe")
    me = lax.axis_index("tensor")
    place = lax.axis_index("seq")
    half = LANES // 2
    wide = 2 * LANES

    core = lax.rem(me, 2)
    chip = me // 2
    partner = me + 1 - 2 * core
    chips = n_tensor // 2
    pieces = near_recv.shape[1]
    some = rows // pieces
    aligned = w_out.ndim == 3

    def chip_at(d):
        return lax.rem(chip + d, chips)

    order = list(range(1, chips)) + [0]
    lending = [(d, 2 * chip_at(d) + 1 - core) for d in order]
    keeping = [(d, 2 * chip_at(d) + core) for d in order]

    def load(src, dst, k):
        return pltpu.make_async_copy(src, dst, w_sem.at[k])

    loads = [
        load(step_hbm.at[0], w_step, 0),
        load(state_hbm.at[0], w_state, 1),
        load(inner_hbm.at[0], w_inner, 2),
        load(gate_hbm.at[0], w_gate, 3),
    ]
    if aligned:
        outs = [
            load(
                out_hbm.at[0, :, pl.ds(pl.multiple_of(j * narrow, LANES), narrow)],
                w_out.at[d, :, pl.ds(side * narrow, narrow)],
                4 + 2 * d + side,
            )
            for pair in zip(lending, keeping)
            for side, (d, j) in enumerate(pair)
        ]
    else:
        outs = [load(out_hbm.at[0], w_out, 4)]
    vectors = [
        pltpu.make_async_copy(src, dst, v_sem.at[k])
        for k, (src, dst) in enumerate(
            (
                (prenorm_hbm, prenorm),
                (inner_taps_hbm, inner_taps),
                (state_taps_hbm, state_taps),
                (step_bias_hbm, step_bias),
                (decay_rate_hbm, decay_rate),
                (skip_scale_hbm, skip_scale),
                (inner_gain_hbm, inner_gain),
            )
        )
    ]

    def stage(m):
        return pltpu.make_async_copy(tokens.at[m], u.at[m, me], t_sem.at[m])

    def at_chip(d):
        return 2 * chip_at(d) + core

    def gather(m, q, src, recv, where):
        block = u.at[m, src, pl.ds(q * some, some)]
        return remote(block, block, ag_send.at[m], recv, {"tensor": where})

    def near(m, q):
        return gather(m, q, me, near_recv.at[m, q], partner)

    def cross(m, d, q):
        return gather(m, q, me, ag_recv.at[m, d - 1, q], at_chip(d))

    def crossed(m, d, q):
        return gather(m, q, at_chip(chips - d), ag_recv.at[m, d - 1, q], partner)

    def hand(m, d, q):
        return gather(m, q, at_chip(chips - d), near_recv.at[m, q], partner)

    def gathered(m, q):
        half_of = u.at[m, pl.ds(0, chips), pl.ds(q * some, some)]
        return remote(half_of, half_of, ag_send.at[m], near_recv.at[m, q], {"tensor": partner})

    def bulk(block, send):
        return remote(block, block, send, near_recv.at[0, 0], {"tensor": partner})

    def send_own(m, q):
        for d in range(1, chips):
            cross(m, d, q).start()
        near(m, q).start()

    groups = [(0, tiles)]

    def rim_copy(m, k):
        at = pl.ds(groups[k][0], groups[k][1] - groups[k][0])
        return remote(
            raw.at[m, at, pl.ds(rows, edge)],
            raw.at[m, at, pl.ds(0, edge)],
            rim_send.at[m, k],
            rim_recv.at[m, k],
            {"seq": lax.rem(place + 1, n_seq)},
        )

    def chain(m, i):
        return remote(
            snd.at[m, i],
            ent.at[m, i],
            ch_send.at[m],
            ch_recv.at[m, i],
            {"seq": lax.rem(place + 1, n_seq)},
        )

    def lend(m, d, j):
        to = chip_at(d)
        return remote(
            term.at[m, j], lent.at[m, to], lend_send.at[m], lend_recv.at[m, to], {"tensor": partner}
        )

    def borrowed(m, d):
        to = chip_at(d)
        return remote(
            lent.at[m, to], lent.at[m, to], lend_send.at[m], lend_recv.at[m, to], {"tensor": partner}
        )

    def part(m, d, q):
        at = pl.ds(q * some, some)
        return remote(
            bundle.at[m, d - 1, at],
            parts.at[m, d - 1, at],
            rs_send.at[m],
            rs_recv.at[m, d - 1, q],
            {"tensor": at_chip(d)},
        )

    def squares(m, j):
        return remote(
            sq_own.at[m], sq_all.at[m, me], sq_send.at[m], sq_recv.at[m], {"tensor": j}
        )

    def squared(m):
        block = sq_all.at[m, pl.ds(0, n_tensor - 1)]
        return remote(block, block, sq_send.at[m], sq_recv.at[m], {"tensor": partner})

    def relay(m, q):
        return remote(
            own.at[m, pl.ds(q * some, some)],
            u.at[m, me, pl.ds(q * some, some)],
            pipe_send.at[m],
            pipe_recv.at[m, q],
            {"pipe": lax.rem(section + 1, n_pipe)},
        )

    def others(action):
        for j in range(n_tensor):
            pl.when(me != j)(functools.partial(action, j))

    @pl.when(section == 0)
    def _():
        stage(0).start()

    for copy in vectors + loads[:1]:
        copy.start()

    @pl.when(section == 0)
    def _():
        for m in range(1, micros):
            stage(m).start()

    barrier = pltpu.get_barrier_semaphore()

    def greet(where):
        pl.semaphore_signal(barrier, inc=1, device_id=where, device_id_type=MESH)

    others(lambda j: greet({"tensor": j}))
    partners = n_tensor - 1
    for axis, index, count in (("seq", place, n_seq), ("pipe", section, n_pipe)):
        pl.when(index > 0)(functools.partial(greet, {axis: index - 1}))
        pl.when(index < count - 1)(functools.partial(greet, {axis: index + 1}))
        partners = partners + jnp.where(index > 0, 1, 0) + jnp.where(index < count - 1, 1, 0)
    pl.semaphore_wait(barrier, partners)

    @pl.when(section == 0)
    def _():
        stage(0).wait()
        for q in range(pieces):
            send_own(0, q)

    for copy in loads[1:]:
        copy.start()

    for copy in outs:
        copy.start()
    for copy in vectors:
        copy.wait()
    inner_taps[...] = inner_taps[...] * 0.5
    state_taps[...] = state_taps[...] * 0.5
    rates[...] = jnp.zeros_like(rates)
    rates[0:1, :heads] = decay_rate[...] * (-LOG2E)
    rates[1:2, :heads] = step_bias[...]
    rates[2:3, :heads] = skip_scale[...]
    sq_acc[...] = jnp.zeros_like(sq_acc)

    @pl.when(place == 0)
    def _():
        for m in range(micros):
            raw[m, :, 0:edge, :] = jnp.zeros((tiles, edge, LANES), F32)
        ent[...] = jnp.zeros_like(ent)

    low = lax.broadcasted_iota(jnp.int32, (rows, LANES), 0)
    lane = lax.broadcasted_iota(jnp.int32, (rows, LANES), 1)
    later = low >= lane
    for k in range(3):
        later3[:, k * rows : (k + 1) * rows] = later.astype(F32).astype(BF16)

    def spreading(columns, size, first):
        k = lax.broadcasted_iota(jnp.int32, (wide, columns), 0)
        at = lax.broadcasted_iota(jnp.int32, (wide, columns), 1) + first
        row = k
        for start in (half, LANES, LANES + half):
            if size == head_size and start != LANES:
                continue
            row = jnp.where(k >= start, k - start, row)
        if size != head_size:
            row = jnp.where(jnp.logical_and(k >= half, k < LANES), LANES, row)
        inside = jnp.logical_and(at >= row * size, at < (row + 1) * size)
        return jnp.where(inside, 1.0, 0.0).astype(BF16)

    def fill_w(t, _):
        at = pl.multiple_of(t * LANES, LANES)
        spread_w[:, pl.ds(at, LANES)] = spreading(LANES, head_size, at)
        return 0

    def fill_c(t, _):
        at = pl.multiple_of(t * LANES, LANES)
        spread_c[:, pl.ds(at, LANES)] = spreading(LANES, rows, at)
        return 0

    lax.fori_loop(0, pairs, fill_w, 0)
    lax.fori_loop(0, heads, fill_c, 0)
    for t in range(pairs):
        cols = slice(t * LANES, (t + 1) * LANES)
        r = lax.broadcasted_iota(jnp.int32, (8, LANES), 0)
        whole = jnp.broadcast_to(rates[2:3], (8, LANES))
        h0 = lax.broadcasted_iota(jnp.int32, (8, LANES), 1)
        row = jnp.zeros((8, LANES), F32)
        for k in range(pack):
            one = jnp.sum(jnp.where(h0 == t * pack + k, whole, 0.0), axis=1, keepdims=True)
            row = jnp.where(h0 >= k * head_size, one, row)
        skips[:, cols] = row[0:1]

    loads[0].wait()
    w_step_t[...] = (
        jnp.concatenate([w_step[...].astype(F32), jnp.zeros((LANES - heads, width), F32)], axis=0)
        .T.astype(BF16)
    )

    def forward_piece(m, q):
        relay(m, q).wait_recv()
        send_own(m, q)

    def forward(m):
        for q in range(pieces):
            forward_piece(m, q)

    def hand_piece(m, q):
        for d in range(1, chips):
            crossed(m, d, q).wait_recv()
            hand(m, d, q).start()

    def hand_over(m):
        for q in range(pieces):
            hand_piece(m, q)

    def take_input(m):
        for q in range(pieces):
            gathered(m, q).wait_recv()
            at = slice(q * some, (q + 1) * some)
            total = jnp.zeros((some, 1), F32)
            for j in range(n_tensor):
                v = u[m, j, at, :].astype(F32)
                total = total + jnp.sum(v * v, axis=1, keepdims=True)
            scale = lax.rsqrt(total / width + EPS)
            for j in range(n_tensor):
                cols = slice(j * narrow, (j + 1) * narrow)
                v = u[m, j, at, :].astype(F32)
                ni[m, at, cols] = (v * scale * prenorm[:, cols]).astype(BF16)

    def multiply(m, first, begin, end, weights):
        for t in range(begin, end, 2):
            stop = min(t + 2, end)
            r = jnp.dot(ni[m], weights[:, t * LANES : stop * LANES], preferred_element_type=F32)
            for k in range(t, stop):
                raw[m, first + k, edge:, :] = r[:, (k - t) * LANES : (k - t + 1) * LANES]

    def send_rim(m, keys):
        @pl.when(place < n_seq - 1)
        def _():
            for k in keys:
                rim_copy(m, k).start()

    def take_rim(m, keys):
        @pl.when(place > 0)
        def _():
            for k in keys:
                rim_copy(m, k).wait_recv()

    def step_sizes(m):
        v = jnp.dot(ni[m], w_step_t[...], preferred_element_type=F32) + rates[1:2]
        step = jnp.maximum(v, 0.0) + jnp.log1p(jnp.exp(-jnp.abs(v)))
        cum = jnp.dot(
            later3[...],
            jnp.concatenate(split(step * rates[0:1], 3), axis=0),
            preferred_element_type=F32,
        )
        fall_t[m] = (cum - jnp.log(step) * LOG2E).T
        weight = jnp.exp2(cum[rows - 1 :] - cum) * step
        both = jnp.concatenate(
            [
                jnp.concatenate(split(weight, 2), axis=1),
                jnp.concatenate(split(jnp.exp2(cum), 2), axis=1),
            ],
            axis=0,
        )
        for t in range(0, pairs, 2):
            cols = slice(t * LANES, min(t + 2, pairs) * LANES)
            r = jnp.dot(both, spread_w[:, cols], preferred_element_type=F32)
            weight_x[m, :, cols] = r[:rows]
            decay_x[m, :, cols] = r[rows:]
        high, mid, last = split(cum, 3)
        last = pltpu.roll(last.astype(F32), half, 1)
        lhs_c[m] = jnp.concatenate([high, (mid.astype(F32) + last).astype(BF16)], axis=1)

    every = range(len(groups))
    early = pairs * 2 // 5 // 2 * 2

    def project(m, steps_first=False):
        if steps_first:
            step_sizes(m)
        multiply(m, pairs, 0, tiles - pairs, w_state)
        multiply(m, 0, 0, pairs, w_inner)
        send_rim(m, every)
        if not steps_first:
            step_sizes(m)

    def gate_some(m, begin, end):
        for t in range(begin, end, 2):
            cols = slice(t * LANES, min(t + 2, end) * LANES)
            r = jnp.dot(ni[m], w_gate[:, cols], preferred_element_type=F32)
            gate[m, :, cols] = half_silu(0.5 * r)

    def project_gate(m):
        gate_some(m, 0, pairs)

    def tile(m, t):
        taps, at = (inner_taps, t) if t < pairs else (state_taps, t - pairs)
        cols = slice(at * LANES, (at + 1) * LANES)
        total = jnp.broadcast_to(taps[reach + 1, :, cols], (rows, LANES))
        for k in range(reach + 1):
            total = total + taps[k, :, cols] * raw[m, t, pl.ds(edge - reach + k, rows), :]
        result = half_silu(total).astype(BF16)
        conv[m, t] = result
        return result

    def convolve_maps(m):
        b = tile(m, pairs)
        c = tile(m, pairs + 1)
        b_t[m] = b.astype(F32).T.astype(BF16)
        found = lax.dot_general(c, b, (((1,), (1,)), ((), ())), preferred_element_type=F32)
        scores[m] = jnp.where(later, found, 0.0)

    def convolve_some(m, begin, end):
        for t in range(begin, end, 2):
            stop = min(t + 2, end)
            weighted = jnp.concatenate(
                [
                    (
                        tile(m, k).astype(F32) * weight_x[m, :, k * LANES : (k + 1) * LANES]
                    ).astype(BF16)
                    for k in range(t, stop)
                ],
                axis=1,
            )
            r = jnp.dot(b_t[m], weighted, preferred_element_type=F32)
            for k in range(t, stop):
                one = r[:, (k - t) * LANES : (k - t + 1) * LANES]
                states[m, k] = one
                snd[m, k] = one.astype(BF16)

        @pl.when(place == 0)
        def _():
            for i in range(begin, end):
                chain(m, i).start()

    middle = pairs // 4 * 2

    def convolve(m, polled=0):
        take_rim(m, every)
        convolve_maps(m)
        convolve_some(m, 0, 2)
        for i in range(min(polled, 2)):
            poll(m, i)
        convolve_some(m, 2, pairs)
        for i in range(2, polled):
            poll(m, i)

    def inside_some(m, begin, end):
        for i in range(begin, end):
            spread = jnp.dot(
                lhs_c[m],
                spread_c[:, i * pack * rows : (i + 1) * pack * rows],
                preferred_element_type=F32,
            )
            mixing = []
            for k in range(pack):
                fall = spread[:, k * rows : (k + 1) * rows] - fall_t[m, pl.ds(i * pack + k, 1), :]
                mixing.append((scores[m] * jnp.exp2(jnp.minimum(fall, CAP))).astype(BF16))
            x = conv[m, i]
            apart = [
                jnp.where(jnp.logical_and(lane >= k * head_size, lane < (k + 1) * head_size), x, 0.0)
                for k in range(pack)
            ]
            result = jnp.dot(
                jnp.concatenate(mixing, axis=1),
                jnp.concatenate([a.astype(BF16) for a in apart], axis=0),
                preferred_element_type=F32,
            )
            cols = slice(i * LANES, (i + 1) * LANES)
            base[m, :, cols] = result + skips[:, cols] * x.astype(F32)

    def inside(m):
        inside_some(m, 0, pairs)

    def poll(m, i):
        @pl.when(place > 0)
        def _():
            chain(m, i).wait_recv()

        @pl.when(jnp.logical_and(place > 0, place < n_seq - 1))
        def _():
            cols = slice(i * LANES, (i + 1) * LANES)
            snd[m, i] = (
                decay_x[m, rows - 1 :, cols] * ent[m, i].astype(F32) + states[m, i]
            ).astype(BF16)
            chain(m, i).start()

    def across(m, t, end):
        entering = jnp.concatenate([ent[m, i] for i in range(t, end)], axis=1)
        cols = slice(t * LANES, end * LANES)
        over = jnp.dot(conv[m, pairs + 1], entering, preferred_element_type=F32)
        gated = (base[m, :, cols] + decay_x[m, :, cols] * over) * gate[m, :, cols]
        squares_of = gated * gated
        total = squares_of[:, :LANES]
        for k in range(1, end - t):
            total = total + squares_of[:, k * LANES : (k + 1) * LANES]
        sq_acc[m] += total
        g[m, :, cols] = (gated * inner_gain[:, cols]).astype(BF16)

    def scan(m, between=(), ready=0, start=0):
        between = dict(between)
        done = 0
        for i in range(pairs):
            if i >= start:
                poll(m, i)
            if i in between:
                between[i]()
            if i >= ready or i == pairs - 1:
                while done + 2 <= i + 1 or (i == pairs - 1 and done <= i):
                    across(m, done, min(done + 2, pairs))
                    done = min(done + 2, pairs)

    def project_out(m):
        if m == 0:
            for copy in outs:
                copy.wait()
        if aligned:
            for d, j in lending:
                if d > 0:
                    r = jnp.dot(g[m], w_out[d, :, :narrow], preferred_element_type=F32)
                    term[m, j] = r.astype(BF16)
                    lend(m, d, j).start()
                    mine[m, d] = jnp.dot(g[m], w_out[d, :, narrow:], preferred_element_type=F32)
                    continue
                r = jnp.dot(g[m], w_out[d], preferred_element_type=F32)
                term[m, j] = r[:, :narrow].astype(BF16)
                lend(m, d, j).start()
                mine[m, d] = r[:, narrow:]
        else:
            for j in range(n_tensor):
                r = jnp.dot(
                    g[m], w_out[:, j * narrow : (j + 1) * narrow], preferred_element_type=F32
                )
                d = lax.rem(j // 2 - chip + chips, chips)
                term[m, j] = r.astype(BF16)
                mine[m, d] = jnp.where(core == j % 2, r, mine[m, d])
            for d, j in lending:
                lend(m, d, j).start()
        total = jnp.sum(sq_acc[m], axis=1, keepdims=True)
        sq_own[m] = jnp.broadcast_to(total, (rows, LANES)).T[:8]
        others(lambda j: squares(m, j).start())

    def combine(m):
        for d in range(1, chips):
            borrowed(m, d).wait_recv()
            for q in range(pieces):
                at = slice(q * some, (q + 1) * some)
                bundle[m, d - 1, at, :] = (
                    mine[m, d, at, :] + lent[m, chip_at(d), at, :].astype(F32)
                ).astype(BF16)
                part(m, d, q).start()

    def scale_rows(m):
        squared(m).wait_recv()
        sq_all[m, me] = sq_own[m]
        total = sq_all[m, 0]
        for j in range(1, n_tensor):
            total = total + sq_all[m, j]
        scale = lax.rsqrt(total / (inner * n_tensor) + EPS)
        sq_acc[m] = jnp.broadcast_to(scale[0:1], (LANES, rows)).T
        borrowed(m, 0).wait_recv()

    def finish_piece(m, q):
        at = slice(q * some, (q + 1) * some)
        for d in range(1, chips):
            part(m, d, q).wait_recv()
        summed = mine[m, 0, at, :] + lent[m, chip, at, :].astype(F32)
        for d in range(1, chips):
            summed = summed + parts[m, d - 1, at, :].astype(F32)
        value = (u[m, me, at, :].astype(F32) + summed * sq_acc[m, at, 0:1]).astype(BF16)
        own[m, at, :] = value
        out[0, m, at, :] = value

        @pl.when(section < n_pipe - 1)
        def _():
            relay(m, q).start()

    def finish(m):
        scale_rows(m)
        for q in range(pieces):
            finish_piece(m, q)

    first = section == 0
    weave = jnp.logical_and(first, place > 0)

    def next_input(m):
        for q in range(pieces):
            send_own(m, q)

    @pl.when(first)
    def _():
        hand_over(0)
        for m in range(1, micros):
            stage(m).wait()
            next_input(m)

    @pl.when(section > 0)
    def _():
        forward(0)
        hand_over(0)

    take_input(0)
    for copy in loads[1:]:
        copy.wait()
    count = tiles - pairs
    third = pairs // 3 // 2 * 2 + 2
    project(0)
    pl.when(jnp.logical_not(weave))(lambda: convolve(0, 1))

    @pl.when(weave)
    def _():
        project_gate(0)
        convolve(0, 1)

    def spread_out(steps, start, stop):
        slots = {}
        for k, step in enumerate(steps):
            slots.setdefault(start + k * (stop - start) // len(steps), []).append(step)

        def run(held):
            for step in held:
                step()

        return {at: functools.partial(run, held) for at, held in slots.items()}

    for m in range(1, micros):
        ahead = m - 1

        def gates(m):
            return [lambda: gate_some(m, 0, third), lambda: gate_some(m, third, pairs)]

        def insides(m):
            return [lambda: inside_some(m, 0, middle), lambda: inside_some(m, middle, pairs)]

        pieces_of = [lambda q=q: finish_piece(ahead, q) for q in range(pieces)]

        def first_piece():
            scale_rows(ahead)
            finish_piece(ahead, 0)

        pieces_of[0] = first_piece

        @pl.when(weave)
        def _():
            hand_over(m)
            work = insides(ahead) + [
                lambda: take_input(m),
                lambda: step_sizes(m),
                lambda: multiply(m, pairs, 0, count, w_state),
                lambda: multiply(m, 0, 0, third, w_inner),
                lambda: (multiply(m, 0, third, pairs, w_inner), send_rim(m, every)),
            ] + gates(m)
            scan(ahead, spread_out(work, 0, pairs - 1), 2, min(ahead + 1, 1))
            project_out(ahead)
            convolve(m)
            combine(ahead)
            slots = {0: [insides(m)[0]], 1: [insides(m)[1]]}
            slots[1].append(lambda: pl.when(place == n_seq - 1)(lambda: finish(ahead)))
            for at, step in zip((3, 5, 7), pieces_of):
                at = min(at, pairs - 1)
                slots.setdefault(at, []).append(
                    lambda step=step: pl.when(place < n_seq - 1)(step)
                )
            scan(
                m,
                {
                    at: (lambda held=held: [step() for step in held])
                    for at, held in slots.items()
                },
                2,
            )
            for step in pieces_of[3:]:
                pl.when(place < n_seq - 1)(step)

        @pl.when(section > 0)
        def _():
            share = pieces // 2

            def forward_some(begin, end):
                for q in range(begin, end):
                    forward_piece(m, q)

            def with_gate(k):
                gates(ahead)[k]()
                forward_some(share + k * share // 2, share + (k + 1) * share // 2)

            events = [
                (0, lambda: forward_some(0, share)),
                (1, lambda: with_gate(0)),
                (2, lambda: with_gate(1)),
                (3, insides(ahead)[0]),
                (5, insides(ahead)[1]),
            ]
            for q in range(pieces):
                events.append((4 + q * 4 // pieces, functools.partial(hand_piece, m, q)))
            events += [(9, lambda: take_input(m)), (9, lambda: project(m, True))]
            events.sort(key=lambda event: event[0])
            for i in range(pairs):
                if i > 0:
                    poll(ahead, i)
                for at, step in events:
                    if at * pairs // 10 == i:
                        step()
            convolve(m, early)

            def cross_over():
                for t in range(0, pairs, 2):
                    across(ahead, t, min(t + 2, pairs))

            work = [
                cross_over,
                lambda: project_out(ahead),
                lambda: combine(ahead),
            ] + gates(m) + insides(m)
            scan(m, spread_out(work, early, pairs - 2), pairs - 2, early)

        @pl.when(jnp.logical_and(first, place == 0))
        def _():
            if ahead == 0:
                project_gate(ahead)
            insides(ahead)[0]()
            hand_over(m)
            insides(ahead)[1]()
            scan(ahead)
            project_out(ahead)
            take_input(m)
            combine(ahead)
            project(m)
            convolve(m)
            for piece in pieces_of[: pieces // 2]:
                piece()
            project_gate(m)
            insides(m)[0]()
            for piece in pieces_of[pieces // 2 :]:
                piece()
            insides(m)[1]()
            scan(m)

    project_out(micros - 1)
    combine(micros - 1)

    def settle(m):
        bulk(u.at[m, pl.ds(0, n_tensor - 1)], ag_send.at[m]).wait_send()
        bulk(lent.at[m], lend_send.at[m]).wait_send()

        @pl.when(place < n_seq - 1)
        def _():
            for k in every:
                rim_copy(m, k).wait_send()
            bulk(snd.at[m], ch_send.at[m]).wait_send()

    def settle_sums(m):
        squared(m).wait_send()
        bulk(bundle.at[m], rs_send.at[m]).wait_send()

        @pl.when(section < n_pipe - 1)
        def _():
            bulk(own.at[m], pipe_send.at[m]).wait_send()

    @pl.when(section > 0)
    def _():
        for m in range(micros - 1):
            finish(m)

    for m in range(micros):
        settle(m)
    for m in range(micros - 1):
        settle_sums(m)
    finish(micros - 1)
    settle_sums(micros - 1)


def shards(sizes, *args):
    tokens, prenorm, gate_w, inner_w, state_w, step_w = args[:6]
    n_pipe, n_tensor, n_seq = sizes
    micros, rows, narrow = tokens.shape
    width = prenorm.shape[1]
    inner = inner_w.shape[2]
    maps = state_w.shape[2]
    heads = step_w.shape[2]
    pairs = inner // LANES
    wide = inner + maps
    step_w = jnp.swapaxes(step_w, 1, 2)
    inner_taps, state_taps = (jnp.swapaxes(a, 0, 1) for a in args[6:8])
    args = (tokens, prenorm, gate_w, inner_w, state_w, step_w, inner_taps, state_taps) + args[8:]
    edge = 8
    chips = n_tensor // 2
    pieces = 4
    vmem = pl.BlockSpec(memory_space=pltpu.VMEM)
    far = pl.BlockSpec(memory_space=pltpu.HBM)
    dma = pltpu.SemaphoreType.DMA
    V = pltpu.VMEM
    return pl.pallas_call(
        functools.partial(kernel, sizes),
        out_shape=pltpu.VMEM((1, micros, rows, narrow), BF16),
        in_specs=[far] * len(args),
        out_specs=vmem,
        scratch_shapes=[
            V((1, width), F32),
            V(inner_taps.shape, F32),
            V(state_taps.shape, F32),
            V((1, heads), F32),
            V((1, heads), F32),
            V((1, heads), F32),
            V((1, inner), F32),
            V((width, inner), BF16),
            V((width, inner), BF16),
            V((width, maps), BF16),
            V((heads, width), BF16),
            V((chips, inner, 2 * narrow) if narrow % LANES == 0 else (inner, width), BF16),
            V((micros, n_tensor, rows, narrow), BF16),
            V((micros, rows, width), BF16),
            V((micros, wide // LANES, edge + rows, LANES), F32),
            V((micros, wide // LANES, rows, LANES), BF16),
            V((micros, rows, inner), F32),
            V((8, LANES), F32),
            V((width, LANES), BF16),
            V((rows, 3 * rows), BF16),
            V((2 * LANES, inner), BF16),
            V((2 * LANES, heads * rows), BF16),
            V((1, inner), F32),
            V((micros, rows, 2 * LANES), BF16),
            V((micros, LANES, rows), F32),
            V((micros, rows, inner), F32),
            V((micros, rows, inner), F32),
            V((micros, LANES, rows), BF16),
            V((micros, rows, rows), F32),
            V((micros, pairs, LANES, LANES), F32),
            V((micros, pairs, LANES, LANES), BF16),
            V((micros, pairs, LANES, LANES), BF16),
            V((micros, rows, inner), F32),
            V((micros, rows, inner), BF16),
            V((micros, rows, LANES), F32),
            V((micros, 8, rows), F32),
            V((micros, n_tensor, 8, rows), F32),
            V((micros, n_tensor, rows, narrow), BF16),
            V((micros, chips, rows, narrow), F32),
            V((micros, chips, rows, narrow), BF16),
            V((micros, chips - 1, rows, narrow), BF16),
            V((micros, chips - 1, rows, narrow), BF16),
            V((micros, rows, narrow), BF16),
            dma((4 + n_tensor,)),
            dma((7,)),
            dma((micros,)),
            dma((micros,)),
            dma((micros, chips - 1, pieces)),
            dma((micros, pieces)),
            dma((micros, 1)),
            dma((micros, 1)),
            dma((micros,)),
            dma((micros, pairs)),
            dma((micros,)),
            dma((micros, chips)),
            dma((micros,)),
            dma((micros, chips - 1, pieces)),
            dma((micros,)),
            dma((micros,)),
            dma((micros,)),
            dma((micros, pieces)),
        ],
        compiler_params=pltpu.CompilerParams(
            collective_id=0, has_side_effects=True, vmem_limit_bytes=60000 * 1024
        ),
    )(*args)


def solution(mesh):
    sizes = (mesh.shape["pipe"], mesh.shape["tensor"], mesh.shape["seq"])
    placed = (
        P(None, "seq", "tensor"),
        P("pipe", None),
        P("pipe", None, "tensor"),
        P("pipe", None, "tensor"),
        P("pipe", None, None),
        P("pipe", None, "tensor"),
        P("pipe", None, "tensor"),
        P("pipe", None, None),
        P("pipe", "tensor"),
        P("pipe", "tensor"),
        P("pipe", "tensor"),
        P("pipe", "tensor"),
        P("pipe", "tensor", None),
    )
    return jax.shard_map(
        functools.partial(shards, sizes),
        mesh=mesh,
        in_specs=placed,
        out_specs=P("pipe", None, "seq", "tensor"),
        check_vma=False,
    )
```
